32 devices in a mesh: dp: 4 (over y, z), ep: 8 (over x, core).
Axes of the slice: x: 4, y: 2, z: 2, core: 2. Of those that a mesh axis runs over, the one named last changes fastest.
The devices are a block of a 4x4x8 slice.
Arguments:
- dy_home: bfloat16 [4096, 1024], P(('dp', 'ep')), parts along dimension 0
- topk_idx: int32 [4096, 8], P(('dp', 'ep')), parts along dimension 0
- slot_idx: int32 [4096, 8], P(('dp', 'ep')), parts along dimension 0
- gates: float32 [4096, 8], P(('dp', 'ep')), parts along dimension 0
- y_back: bfloat16 [4096, 8, 1024], P(('dp', 'ep')), parts along dimension 0
- x_disp: bfloat16 [128, 512, 1024], P(('dp', 'ep')), parts along dimension 0
- h1_disp: bfloat16 [128, 512, 512], P(('dp', 'ep')), parts along dimension 0
- h3_disp: bfloat16 [128, 512, 512], P(('dp', 'ep')), parts along dimension 0
- w_gate: bfloat16 [32, 1024, 512], P('ep')
- w_up: bfloat16 [32, 1024, 512], P('ep')
- w_down: bfloat16 [32, 512, 1024], P('ep')
Outputs:
- output 1: bfloat16 [4096, 1024], P(('dp', 'ep')), parts along dimension 0
- output 2: float32 [4096, 8], P(('dp', 'ep')), parts along dimension 0
- output 3: float32 [128, 1024, 512], P(('dp', 'ep')), parts along dimension 0
- output 4: float32 [128, 1024, 512], P(('dp', 'ep')), parts along dimension 0
- output 5: float32 [128, 512, 1024], P(('dp', 'ep')), parts along dimension 0
There are 4 independent parts. The reference program is written for one: setup_inputs(seed, part) draws one part's arguments, and reference() takes and returns one part's arrays. A program takes and returns all parts, laid end to end along the dimension named above; an argument that names none is the same for every part.
All inputs are finite; a program needn't handle non-finite values.
Results may differ from the reference program's by a relative error of at most 0.0149677.
Values are sent between devices in bfloat16 or wider.
A program may use at most 768 MiB of HBM per device.

```python
import jax
import jax.numpy as jnp
from jax import lax

EP_SIZE = 8
TOKENS_DEV = 128
TOP = 8
EXPERTS = 32
D = 1024
FF = 512

CAPACITY = 2 * TOKENS_DEV * TOP // EXPERTS
ALL_TOKENS = EP_SIZE * TOKENS_DEV
ROWS_ALL = EXPERTS * EP_SIZE * CAPACITY


def rank_in_buffer(expert_ids):
    num_items = TOKENS_DEV * TOP
    positions = jnp.arange(num_items, dtype=jnp.int32)
    sort_order = jnp.argsort(expert_ids * num_items + positions)
    sorted_ids = expert_ids[sort_order]
    first_pos = jnp.searchsorted(sorted_ids, sorted_ids, side='left').astype(jnp.int32)
    buf_rank = jnp.zeros((num_items,), jnp.int32).at[sort_order].set(positions - first_pos)
    return jnp.where(buf_rank < CAPACITY, buf_rank, -1)


def route_draw(route_key):
    key_base, key_bias, key_hot = jax.random.split(route_key, 3)
    base_score = jax.random.randint(key_base, (ALL_TOKENS, EXPERTS), 0, 65536)
    expert_bias = jax.random.randint(key_bias, (EXPERTS,), 0, 32768)
    hot_expert = jax.random.randint(key_hot, (), 0, EXPERTS)
    tok_pos = jnp.arange(ALL_TOKENS, dtype=jnp.int32) % TOKENS_DEV
    expert_ids = jnp.arange(EXPERTS, dtype=jnp.int32)
    forced = (tok_pos[:, None] <= CAPACITY) & (expert_ids[None, :] == hot_expert)
    full_score = (base_score + expert_bias[None, :] + jnp.where(forced, 131072, 0)) * EXPERTS + expert_ids[None, :]
    topk_idx = lax.top_k(full_score, TOP)[1].astype(jnp.int32)
    slot_idx = jax.vmap(rank_in_buffer)(topk_idx.reshape(EP_SIZE, TOKENS_DEV * TOP))
    return topk_idx, slot_idx.reshape(ALL_TOKENS, TOP)


def buffer_index(topk_idx, slot_idx):
    src_dev = jnp.arange(ALL_TOKENS, dtype=jnp.int32) // TOKENS_DEV
    flat_pos = (topk_idx * EP_SIZE + src_dev[:, None]) * CAPACITY + slot_idx
    return jnp.where(slot_idx >= 0, flat_pos, ROWS_ALL)


def expert_forward(operands):
    x_expert, gate_w, up_w, down_w = operands
    h_gate = jnp.dot(x_expert, gate_w, preferred_element_type=jnp.float32).astype(jnp.bfloat16)
    h_up = jnp.dot(x_expert, up_w, preferred_element_type=jnp.float32).astype(jnp.bfloat16)
    hidden_act = (jax.nn.silu(h_gate.astype(jnp.float32)) * h_up.astype(jnp.float32)).astype(jnp.bfloat16)
    y_expert = jnp.dot(hidden_act, down_w, preferred_element_type=jnp.float32).astype(jnp.bfloat16)
    return h_gate, h_up, y_expert


def forward_buffers(x_tok, flat_pos, w_gate, w_up, w_down):
    x_rows = jnp.broadcast_to(x_tok[:, None, :], (ALL_TOKENS, TOP, D)).reshape(ALL_TOKENS * TOP, D)
    x_disp = jnp.zeros((ROWS_ALL, D), jnp.bfloat16).at[flat_pos.reshape(-1)].set(x_rows, mode='drop')
    x_disp = x_disp.reshape(EXPERTS, EP_SIZE * CAPACITY, D)
    h1_disp, h3_disp, y_disp = lax.map(expert_forward, (x_disp, w_gate, w_up, w_down))
    y_back = jnp.take(y_disp.reshape(ROWS_ALL, D), flat_pos, axis=0, mode='fill', fill_value=0)
    return y_back, x_disp, h1_disp, h3_disp


def setup_inputs(seed: int = 0, part: int = 0) -> dict:
    root_key = jax.random.key(seed)
    key_gate, key_up, key_down = jax.random.split(root_key, 3)
    w_gate = (jax.random.normal(key_gate, (EXPERTS, D, FF), jnp.float32) * D ** -0.5).astype(jnp.bfloat16)
    w_up = (jax.random.normal(key_up, (EXPERTS, D, FF), jnp.float32) * D ** -0.5).astype(jnp.bfloat16)
    w_down = (jax.random.normal(key_down, (EXPERTS, FF, D), jnp.float32) * FF ** -0.5).astype(jnp.bfloat16)
    part_key = jax.random.fold_in(root_key, part)
    key_route, key_tok, key_grad, key_mix = jax.random.split(part_key, 4)
    topk_idx, slot_idx = route_draw(key_route)
    gates = jax.random.uniform(key_mix, (ALL_TOKENS, TOP), jnp.float32, 0.2, 1.0)
    x_tok = jax.random.normal(key_tok, (ALL_TOKENS, D), jnp.float32).astype(jnp.bfloat16)
    dy_home = jax.random.normal(key_grad, (ALL_TOKENS, D), jnp.float32).astype(jnp.bfloat16)
    flat_pos = buffer_index(topk_idx, slot_idx)
    y_back, x_disp, h1_disp, h3_disp = forward_buffers(x_tok, flat_pos, w_gate, w_up, w_down)
    return {'dy_home': dy_home, 'topk_idx': topk_idx, 'slot_idx': slot_idx, 'gates': gates,
            'y_back': y_back, 'x_disp': x_disp, 'h1_disp': h1_disp, 'h3_disp': h3_disp,
            'w_gate': w_gate, 'w_up': w_up, 'w_down': w_down}


def expert_backward(operands):
    dy_expert, x_expert, h_gate, h_up, gate_w, up_w, down_w = operands
    gate_f = h_gate.astype(jnp.float32)
    up_f = h_up.astype(jnp.float32)
    sig_gate = jax.nn.sigmoid(gate_f)
    silu_g = gate_f * sig_gate
    hidden_act = (silu_g * up_f).astype(jnp.bfloat16)
    d_act = jnp.dot(dy_expert, down_w.T, preferred_element_type=jnp.float32).astype(jnp.bfloat16).astype(jnp.float32)
    dh_gate = (d_act * up_f * sig_gate * (1.0 + gate_f * (1.0 - sig_gate))).astype(jnp.bfloat16)
    dh_up = (d_act * silu_g).astype(jnp.bfloat16)
    dw_down = jnp.dot(hidden_act.T, dy_expert, preferred_element_type=jnp.float32)
    dw_gate = jnp.dot(x_expert.T, dh_gate, preferred_element_type=jnp.float32)
    dw_up = jnp.dot(x_expert.T, dh_up, preferred_element_type=jnp.float32)
    dx_expert = (jnp.dot(dh_gate, gate_w.T, preferred_element_type=jnp.float32)
                 + jnp.dot(dh_up, up_w.T, preferred_element_type=jnp.float32)).astype(jnp.bfloat16)
    return dx_expert, dw_gate, dw_up, dw_down


def reference(dy_home, topk_idx, slot_idx, gates, y_back, x_disp, h1_disp, h3_disp, w_gate, w_up, w_down):
    d_gates = jnp.einsum('td,tjd->tj', dy_home.astype(jnp.float32), y_back.astype(jnp.float32))
    flat_pos = buffer_index(topk_idx, slot_idx)
    gated_rows = (gates[:, :, None] * dy_home[:, None, :].astype(jnp.float32)).astype(jnp.bfloat16)
    dy_disp = jnp.zeros((ROWS_ALL, D), jnp.bfloat16).at[flat_pos.reshape(-1)].set(gated_rows.reshape(ALL_TOKENS * TOP, D), mode='drop')
    dy_disp = dy_disp.reshape(EXPERTS, EP_SIZE * CAPACITY, D)
    dx_disp, dw_gate, dw_up, dw_down = lax.map(expert_backward, (dy_disp, x_disp, h1_disp, h3_disp, w_gate, w_up, w_down))
    returned = jnp.take(dx_disp.reshape(ROWS_ALL, D), flat_pos, axis=0, mode='fill', fill_value=0)
    dx_home = jnp.sum(returned.astype(jnp.float32), axis=1).astype(jnp.bfloat16)
    return dx_home, d_gates, dw_gate, dw_up, dw_down
```

```python
import functools
import jax
import jax.numpy as jnp
from jax import lax
from jax.experimental import pallas as pl
from jax.experimental.pallas import tpu as pltpu
from jax.sharding import PartitionSpec as P

MESH = pl.DeviceIdType.MESH
F32 = jnp.float32
BF16 = jnp.bfloat16


def dot_nt(a, b):
    return lax.dot_general(a, b, (((1,), (1,)), ((), ())), preferred_element_type=F32)


def dot_tn(a, b):
    return lax.dot_general(a, b, (((0,), (0,)), ((), ())), preferred_element_type=F32)


def exchange_kernel(ep, cap, dy_hbm, topk_ref, slot_ref, gate_ref, yb_hbm, h1_hbm, h3_hbm, wg_hbm, wu_hbm, wd_hbm,
                    dx_ref, dg_ref, dyd_hbm, act_hbm, dh1_hbm, dh3_hbm,
                    dyall, meta, square, yb_v, h1_v, h3_v, wg_v, wu_v, wd_v, dyd_v, act_v, dh1_v, dh3_v,
                    onehot, dxd, mine, theirs, got, relay, final,
                    load_sem, meta_send, meta_recv, dy_send, dy_recv, d2d_send, d2d_recv, part_send, part_recv,
                    ring_send, ring_recv, out_sem):
    chips = ep // 2
    tok, width = dyall.shape[1], dyall.shape[2]
    half = tok // 2
    n_exp = wd_v.shape[0]
    top = topk_ref.shape[1]
    me = lax.axis_index('ep')
    chip, core = me // 2, me % 2
    right = (chip + 1) % chips
    left = (chip + chips - 1) % chips
    far = (chip + 2) % chips
    dev_r, dev_l, dev_p = right * 2 + core, left * 2 + core, chip * 2 + (1 - core)
    home_f = far * 2 + core

    def remote(src, dst, send_sem, recv_sem, dev):
        return pltpu.make_async_remote_copy(src_ref=src, dst_ref=dst, send_sem=send_sem, recv_sem=recv_sem,
                                            device_id={'ep': dev}, device_id_type=MESH)

    loads = [pltpu.make_async_copy(src, dst, load_sem.at[i]) for i, (src, dst) in enumerate((
        (dy_hbm, dyall.at[me]), (wd_hbm, wd_v), (h1_hbm, h1_v), (h3_hbm, h3_v), (wg_hbm, wg_v), (wu_hbm, wu_v),
        (yb_hbm, yb_v)))]
    for copy in loads:
        copy.start()

    slot = slot_ref[...]
    pos = jnp.where(slot >= 0, topk_ref[...] * cap + slot, -1).astype(F32)
    square[...] = jnp.zeros_like(square)
    square[:, 0:top] = pos
    square[:, top:2 * top] = gate_ref[...]
    meta[me] = square[...].T[0:2 * top, :]

    barrier = pltpu.get_barrier_semaphore()
    for d in range(1, ep):
        pl.semaphore_signal(barrier, inc=1, device_id={'ep': (me + d) % ep}, device_id_type=MESH)
    pl.semaphore_wait(barrier, ep - 1)

    metas = [remote(meta.at[me], meta.at[me], meta_send.at[d - 1], meta_recv.at[d - 1], (me + d) % ep)
             for d in range(1, ep)]
    for copy in metas:
        copy.start()
    loads[0].wait()

    def rows(home, h):
        return dyall.at[home, pl.ds(h * half, half), :]

    own_p = remote(dyall.at[me], dyall.at[me], d2d_send.at[0], d2d_recv.at[0], dev_p)
    own_p.start()
    r_0 = remote(rows(me, 0), rows(me, 0), dy_send.at[0], dy_recv.at[0], dev_r)
    l_1 = remote(rows(me, 1), rows(me, 1), dy_send.at[1], dy_recv.at[1], dev_l)
    r_1 = remote(rows(me, 1), rows(me, 1), dy_send.at[2], dy_recv.at[2], dev_r)
    l_0 = remote(rows(me, 0), rows(me, 0), dy_send.at[3], dy_recv.at[3], dev_l)
    for copy in (r_0, l_1, r_1, l_0):
        copy.start()
    f_0 = remote(rows(dev_l, 0), rows(dev_l, 0), dy_send.at[4], dy_recv.at[4], dev_r)
    f_1 = remote(rows(dev_r, 1), rows(dev_r, 1), dy_send.at[5], dy_recv.at[5], dev_l)
    left_p = remote(dyall.at[dev_l], dyall.at[dev_l], d2d_send.at[1], d2d_recv.at[1], dev_p)
    right_p = remote(dyall.at[dev_r], dyall.at[dev_r], d2d_send.at[2], d2d_recv.at[2], dev_p)
    far_p = remote(dyall.at[home_f], dyall.at[home_f], d2d_send.at[3], d2d_recv.at[3], dev_p)

    def build(home, chip_q, hc):
        table = meta[home]
        row_id = lax.broadcasted_iota(jnp.int32, (n_exp * cap, tok), 0).astype(F32) + (me * (n_exp * cap)).astype(F32)
        hit = jnp.zeros((n_exp * cap, tok), F32)
        gate = jnp.zeros((n_exp * cap, tok), F32)
        for j in range(top):
            same = row_id == table[j:j + 1, :]
            hit = jnp.where(same, 1.0, hit)
            gate = jnp.where(same, table[top + j:top + j + 1, :], gate)
        gate_row = jnp.sum(gate, axis=1, keepdims=True)
        sel = hit.astype(BF16)
        onehot[hc] = sel
        base = chip_q * (2 * cap) + hc * cap
        for n in range(width // 256):
            cols = slice(n * 256, (n + 1) * 256)
            block = (jnp.dot(sel, dyall[home, :, cols], preferred_element_type=F32) * gate_row).astype(BF16)
            for e in range(n_exp):
                dyd_v[e, pl.ds(base, cap), cols] = block[e * cap:(e + 1) * cap]

    def experts(chip_q):
        span = pl.ds(chip_q * (2 * cap), 2 * cap)

        def one(e, carry):
            d_act = dot_nt(dyd_v[e, span, :], wd_v[e]).astype(BF16).astype(F32)
            gate_f = h1_v[e, span, :].astype(F32)
            up_f = h3_v[e, span, :].astype(F32)
            sig = jax.nn.sigmoid(gate_f)
            silu = gate_f * sig
            act_v[e, span, :] = (silu * up_f).astype(BF16)
            dh1 = (d_act * up_f * sig * (1.0 + gate_f * (1.0 - sig))).astype(BF16)
            dh3 = (d_act * silu).astype(BF16)
            dh1_v[e, span, :] = dh1
            dh3_v[e, span, :] = dh3
            out = (dot_nt(dh1, wg_v[e]) + dot_nt(dh3, wu_v[e])).astype(BF16)
            at = pl.ds(pl.multiple_of(e * cap, cap), cap)
            dxd[0, at, :] = out[0:cap]
            dxd[1, at, :] = out[cap:2 * cap]
            return carry
        lax.fori_loop(0, n_exp, one, 0)

    def combine(chip_q):
        theirs[chip_q] = dot_tn(onehot[1 - core], dxd[1 - core])
        mine[chip_q] = dot_tn(onehot[core], dxd[core])

    def chunk(chip_q):
        for hc in range(2):
            build(chip_q * 2 + hc, chip_q, hc)
        experts(chip_q)
        combine(chip_q)

    parts = {}

    def send_part(name, i, chip_q):
        parts[name] = remote(theirs.at[chip_q], got.at[chip_q], part_send.at[i], part_recv.at[i], dev_p)
        parts[name].start()

    def add_part(name, chip_q):
        parts[name].wait_recv()
        mine[chip_q] = mine[chip_q] + got[chip_q]

    for copy in metas:
        copy.wait_recv()
    own_p.wait_recv()
    for copy in loads[1:6]:
        copy.wait()
    chunk(chip)
    r_0.wait_recv()
    f_0.start()
    l_1.wait_recv()
    f_1.start()
    send_part('own', 0, chip)

    loads[6].wait()

    def gate_grad(i, carry):
        at = pl.ds(pl.multiple_of(i * 16, 16), 16)
        prod = yb_v[at].astype(F32) * dyall[me, at, :].astype(F32)[:, None, :]
        dg_ref[at, :] = jnp.sum(prod, axis=-1)
        return carry
    lax.fori_loop(0, tok // 16, gate_grad, 0)

    r_1.wait_recv()
    left_p.start()
    l_0.wait_recv()
    right_p.start()
    left_p.wait_recv()
    chunk(left)
    send_part('left', 1, left)
    right_p.wait_recv()
    chunk(right)
    send_part('right', 2, right)
    f_0.wait_recv()
    f_1.wait_recv()
    far_p.start()
    add_part('left', left)
    add_part('right', right)

    def piece(ref, h):
        return ref.at[pl.ds(h * half, half), :]

    one_r = remote(piece(mine.at[right], 1), piece(final.at[0], 1), ring_send.at[0], ring_recv.at[0], dev_r)
    one_l = remote(piece(mine.at[left], 0), piece(final.at[1], 0), ring_send.at[1], ring_recv.at[1], dev_l)
    one_r.start()
    one_l.start()
    far_p.wait_recv()
    chunk(far)
    send_part('far', 3, far)
    outs = [pltpu.make_async_copy(src, dst, out_sem.at[i]) for i, (src, dst) in enumerate((
        (dyd_v, dyd_hbm), (act_v, act_hbm), (dh1_v, dh1_hbm), (dh3_v, dh3_hbm)))]
    for copy in outs:
        copy.start()
    add_part('far', far)
    two_r = remote(piece(mine.at[far], 0), relay.at[0], ring_send.at[2], ring_recv.at[2], dev_r)
    two_l = remote(piece(mine.at[far], 1), relay.at[1], ring_send.at[3], ring_recv.at[3], dev_l)
    two_r.start()
    two_l.start()
    add_part('own', chip)
    two_r.wait_recv()
    mine[right, 0:half, :] = mine[right, 0:half, :] + relay[0]
    two_l.wait_recv()
    mine[left, half:tok, :] = mine[left, half:tok, :] + relay[1]
    three_r = remote(piece(mine.at[right], 0), piece(final.at[0], 0), ring_send.at[4], ring_recv.at[4], dev_r)
    three_l = remote(piece(mine.at[left], 1), piece(final.at[1], 1), ring_send.at[5], ring_recv.at[5], dev_l)
    three_r.start()
    three_l.start()
    for copy in (one_r, one_l, three_r, three_l):
        copy.wait_recv()
    dx_ref[...] = (mine[chip] + final[0] + final[1]).astype(BF16)

    for copy in metas + [own_p, r_0, l_1, r_1, l_0, f_0, f_1, left_p, right_p, far_p] + list(parts.values()) + [
            one_r, one_l, two_r, two_l, three_r, three_l]:
        copy.wait_send()
    for copy in outs:
        copy.wait()


def exchange(ep, dy, topk, slot, gates, y_back, h1, h3, w_gate, w_up, w_down):
    tok, width = dy.shape
    n_exp, rows_e, ff = h1.shape
    cap = rows_e // ep
    chips = ep // 2
    top = topk.shape[1]
    any_spec = pl.BlockSpec(memory_space=pl.ANY)
    vmem_spec = pl.BlockSpec(memory_space=pltpu.VMEM)
    dma = pltpu.SemaphoreType.DMA
    return pl.pallas_call(
        functools.partial(exchange_kernel, ep, cap),
        out_shape=(
            jax.ShapeDtypeStruct((tok, width), BF16),
            jax.ShapeDtypeStruct((tok, top), F32),
            jax.ShapeDtypeStruct((n_exp, rows_e, width), BF16),
            jax.ShapeDtypeStruct((n_exp, rows_e, ff), BF16),
            jax.ShapeDtypeStruct((n_exp, rows_e, ff), BF16),
            jax.ShapeDtypeStruct((n_exp, rows_e, ff), BF16),
        ),
        in_specs=[any_spec, vmem_spec, vmem_spec, vmem_spec] + [any_spec] * 6,
        out_specs=(vmem_spec, vmem_spec) + (any_spec,) * 4,
        scratch_shapes=[
            pltpu.VMEM((ep, tok, width), BF16),
            pltpu.VMEM((ep, 2 * top, tok), F32),
            pltpu.VMEM((tok, tok), F32),
            pltpu.VMEM((tok, top, width), BF16),
            pltpu.VMEM((n_exp, rows_e, ff), BF16),
            pltpu.VMEM((n_exp, rows_e, ff), BF16),
            pltpu.VMEM((n_exp, width, ff), BF16),
            pltpu.VMEM((n_exp, width, ff), BF16),
            pltpu.VMEM((n_exp, ff, width), BF16),
            pltpu.VMEM((n_exp, rows_e, width), BF16),
            pltpu.VMEM((n_exp, rows_e, ff), BF16),
            pltpu.VMEM((n_exp, rows_e, ff), BF16),
            pltpu.VMEM((n_exp, rows_e, ff), BF16),
            pltpu.VMEM((2, n_exp * cap, tok), BF16),
            pltpu.VMEM((2, n_exp * cap, width), BF16),
            pltpu.VMEM((chips, tok, width), F32),
            pltpu.VMEM((chips, tok, width), F32),
            pltpu.VMEM((chips, tok, width), F32),
            pltpu.VMEM((2, tok // 2, width), F32),
            pltpu.VMEM((2, tok, width), F32),
            dma((7,)), dma((ep - 1,)), dma((ep - 1,)), dma((6,)), dma((6,)), dma((4,)), dma((4,)),
            dma((4,)), dma((4,)), dma((6,)), dma((6,)), dma((4,)),
        ],
        compiler_params=pltpu.CompilerParams(collective_id=0, has_side_effects=True, vmem_limit_bytes=60 * 2**20),
        name='exchange',
    )(dy, topk, slot, gates, y_back, h1, h3, w_gate, w_up, w_down)


def weight_grad_kernel(x_ref, dyd_ref, act_ref, dh1_ref, dh3_ref, dwg_ref, dwu_ref, dwd_ref):
    dwd_ref[0] = dot_tn(act_ref[0], dyd_ref[0])
    dwg_ref[0] = dot_tn(x_ref[0], dh1_ref[0])
    dwu_ref[0] = dot_tn(x_ref[0], dh3_ref[0])


def weight_grads(x, dyd, act, dh1, dh3):
    n_exp, rows_e, width = x.shape
    ff = act.shape[2]
    wide = pl.BlockSpec((1, rows_e, width), lambda e: (e, 0, 0))
    thin = pl.BlockSpec((1, rows_e, ff), lambda e: (e, 0, 0))
    tall = pl.BlockSpec((1, width, ff), lambda e: (e, 0, 0))
    flat = pl.BlockSpec((1, ff, width), lambda e: (e, 0, 0))
    return pl.pallas_call(
        weight_grad_kernel,
        grid=(n_exp,),
        out_shape=(
            jax.ShapeDtypeStruct((n_exp, width, ff), F32),
            jax.ShapeDtypeStruct((n_exp, width, ff), F32),
            jax.ShapeDtypeStruct((n_exp, ff, width), F32),
        ),
        in_specs=[wide, wide, thin, thin, thin],
        out_specs=(tall, tall, flat),
        compiler_params=pltpu.CompilerParams(vmem_limit_bytes=48 * 2**20),
        name='weight_grads',
    )(x, dyd, act, dh1, dh3)


def solution(mesh):
    ep = mesh.shape['ep']
    tok_spec = P(('dp', 'ep'), None)
    buf_spec = P(('dp', 'ep'), None, None)
    expert_spec = P('ep', None, None)

    def device_step(dy, topk_idx, slot_idx, gates, y_back, x_disp, h1_disp, h3_disp, w_gate, w_up, w_down):
        dx, d_gates, dyd, act, dh1, dh3 = exchange(
            ep, dy, topk_idx, slot_idx, gates, y_back, h1_disp, h3_disp, w_gate, w_up, w_down)
        dw_gate, dw_up, dw_down = weight_grads(x_disp, dyd, act, dh1, dh3)
        return dx, d_gates, dw_gate, dw_up, dw_down

    return jax.shard_map(
        device_step, mesh=mesh,
        in_specs=(tok_spec, tok_spec, tok_spec, tok_spec, buf_spec, buf_spec, buf_spec, buf_spec,
                  expert_spec, expert_spec, expert_spec),
        out_specs=(tok_spec, tok_spec, buf_spec, buf_spec, buf_spec),
        check_vma=False)
```

```python
import functools
import jax
import jax.numpy as jnp
from jax import lax
from jax.experimental import pallas as pl
from jax.experimental.pallas import tpu as pltpu
from jax.sharding import PartitionSpec as P

MESH = pl.DeviceIdType.MESH
F32 = jnp.float32
BF16 = jnp.bfloat16


def dot_nt(a, b):
    return lax.dot_general(a, b, (((1,), (1,)), ((), ())), preferred_element_type=F32)


def dot_tn(a, b):
    return lax.dot_general(a, b, (((0,), (0,)), ((), ())), preferred_element_type=F32)


def exchange_kernel(ep, cap, dy_hbm, topk_ref, slot_ref, gate_ref, yb_hbm, x_hbm, h1_hbm, h3_hbm, wg_hbm, wu_hbm, wd_hbm,
                    dx_ref, dg_ref, x_v, dyd_v, act_v, dh1_v, dh3_v,
                    dyall, meta, square, yb_v, h1_v, h3_v, silu_v, slope_v, wg_v, wu_v, wd_v,
                    onehot, dxd, mine, theirs, got, relay, final,
                    load_sem, row_sem, meta_send, meta_recv, dy_send, dy_recv, d2d_send, d2d_recv, part_send, part_recv,
                    ring_send, ring_recv):
    chips = ep // 2
    tok, width = dyall.shape[1], dyall.shape[2]
    half = tok // 2
    n_exp = wd_v.shape[0]
    top = topk_ref.shape[0]
    pair = 2 * cap
    me = lax.axis_index('ep')
    chip, core = me // 2, me % 2
    right = (chip + 1) % chips
    left = (chip + chips - 1) % chips
    far = (chip + 2) % chips
    dev_r, dev_l, dev_p = right * 2 + core, left * 2 + core, chip * 2 + (1 - core)
    home_f = far * 2 + core
    chip_at = (chip, left, right, far)

    def remote(src, dst, send_sem, recv_sem, dev):
        return pltpu.make_async_remote_copy(src_ref=src, dst_ref=dst, send_sem=send_sem, recv_sem=recv_sem,
                                            device_id={'ep': dev}, device_id_type=MESH)

    def by_rows(src, dst, i):
        return [pltpu.make_async_copy(src.at[:, pl.ds(chip_at[p] * pair, pair), :],
                                      dst.at[:, pl.ds(p * pair, pair), :], row_sem.at[i, p]) for p in range(chips)]

    own_load = pltpu.make_async_copy(dy_hbm, dyall.at[me], load_sem.at[0])
    h_loads = by_rows(h1_hbm, h1_v, 0) + by_rows(h3_hbm, h3_v, 1)
    w_loads = [pltpu.make_async_copy(src, dst, load_sem.at[i + 1]) for i, (src, dst) in enumerate((
        (wd_hbm, wd_v), (wg_hbm, wg_v), (wu_hbm, wu_v)))]
    yb_load = pltpu.make_async_copy(yb_hbm, yb_v, load_sem.at[4])
    x_loads = by_rows(x_hbm, x_v, 2)
    for copy in [own_load] + h_loads + w_loads + [yb_load] + x_loads:
        copy.start()

    slot = slot_ref[...]
    meta[me, 0:top, :] = jnp.where(slot >= 0, topk_ref[...] * cap + slot, -1).astype(F32)
    meta[me, top:2 * top, :] = gate_ref[...]
    square[...] = jnp.zeros_like(square)

    barrier = pltpu.get_barrier_semaphore()
    for d in range(1, ep):
        pl.semaphore_signal(barrier, inc=1, device_id={'ep': (me + d) % ep}, device_id_type=MESH)
    pl.semaphore_wait(barrier, ep - 1)

    own_load.wait()

    def rows(home, h):
        return dyall.at[home, pl.ds(h * half, half), :]

    r_0 = remote(rows(me, 0), rows(me, 0), dy_send.at[0], dy_recv.at[0], dev_r)
    l_1 = remote(rows(me, 1), rows(me, 1), dy_send.at[1], dy_recv.at[1], dev_l)
    r_1 = remote(rows(me, 1), rows(me, 1), dy_send.at[2], dy_recv.at[2], dev_r)
    l_0 = remote(rows(me, 0), rows(me, 0), dy_send.at[3], dy_recv.at[3], dev_l)
    own_p = remote(dyall.at[me], dyall.at[me], d2d_send.at[0], d2d_recv.at[0], dev_p)
    metas = [remote(meta.at[me], meta.at[me], meta_send.at[d - 1], meta_recv.at[d - 1], (me + d) % ep)
             for d in range(1, ep)]
    for copy in [r_0, l_1, own_p] + metas + [r_1, l_0]:
        copy.start()
    f_0 = remote(rows(dev_l, 0), rows(dev_l, 0), dy_send.at[4], dy_recv.at[4], dev_r)
    f_1 = remote(rows(dev_r, 1), rows(dev_r, 1), dy_send.at[5], dy_recv.at[5], dev_l)
    left_p = remote(dyall.at[dev_l], dyall.at[dev_l], d2d_send.at[1], d2d_recv.at[1], dev_p)
    right_p = remote(dyall.at[dev_r], dyall.at[dev_r], d2d_send.at[2], d2d_recv.at[2], dev_p)
    far_p = remote(dyall.at[home_f], dyall.at[home_f], d2d_send.at[3], d2d_recv.at[3], dev_p)

    def factors(e, carry):
        for p in range(chips):
            span = slice(p * pair, (p + 1) * pair)
            gate_f = h1_v[e, span, :].astype(F32)
            up_f = h3_v[e, span, :].astype(F32)
            sig = jax.nn.sigmoid(gate_f)
            silu = gate_f * sig
            act_v[e, span, :] = (silu * up_f).astype(BF16)
            silu_v[e, span, :] = silu
            slope_v[e, span, :] = up_f * sig * (1.0 + gate_f * (1.0 - sig))
        return carry

    def build(p, hc):
        home = chip_at[p] * 2 + hc
        table = meta[home]
        row_id = lax.broadcasted_iota(jnp.int32, (n_exp * cap, tok), 0).astype(F32) + (me * (n_exp * cap)).astype(F32)
        hit = jnp.zeros((n_exp * cap, tok), F32)
        gate = jnp.zeros((n_exp * cap, tok), F32)
        for j in range(top):
            same = row_id == table[j:j + 1, :]
            hit = jnp.where(same, 1.0, hit)
            gate = jnp.where(same, table[top + j:top + j + 1, :], gate)
        gate_row = jnp.sum(gate, axis=1, keepdims=True)
        sel = hit.astype(BF16)
        onehot[p, hc] = sel
        base = p * pair + hc * cap
        for n in range(width // 256):
            cols = slice(n * 256, (n + 1) * 256)
            block = (jnp.dot(sel, dyall[home, :, cols], preferred_element_type=F32) * gate_row).astype(BF16)
            for e in range(n_exp):
                dyd_v[e, base:base + cap, cols] = block[e * cap:(e + 1) * cap]

    def experts(p, count):
        span = slice(p * pair, (p + count) * pair)
        for e in range(n_exp):
            d_act = dot_nt(dyd_v[e, span, :], wd_v[e]).astype(BF16).astype(F32)
            dh1 = (d_act * slope_v[e, span, :]).astype(BF16)
            dh3 = (d_act * silu_v[e, span, :]).astype(BF16)
            dh1_v[e, span, :] = dh1
            dh3_v[e, span, :] = dh3
            out = (dot_nt(dh1, wg_v[e]) + dot_nt(dh3, wu_v[e])).astype(BF16)
            for q in range(2 * count):
                dxd[p + q // 2, q % 2, e * cap:(e + 1) * cap, :] = out[q * cap:(q + 1) * cap]

    def combine(p):
        theirs[p] = dot_tn(onehot[p, 1 - core], dxd[p, 1 - core])
        mine[p] = dot_tn(onehot[p, core], dxd[p, core])

    parts = [remote(theirs.at[p], got.at[p], part_send.at[p], part_recv.at[p], dev_p) for p in range(chips)]

    def add_part(p):
        parts[p].wait_recv()
        mine[p] = mine[p] + got[p]

    for copy in h_loads:
        copy.wait()
    lax.fori_loop(0, n_exp, factors, 0)
    r_0.wait_recv()
    f_0.start()
    l_1.wait_recv()
    f_1.start()
    for copy in metas:
        copy.wait_recv()
    own_p.wait_recv()
    for hc in range(2):
        build(0, hc)
    for copy in w_loads:
        copy.wait()
    experts(0, 1)
    r_1.wait_recv()
    left_p.start()
    l_0.wait_recv()
    right_p.start()
    combine(0)
    parts[0].start()
    left_p.wait_recv()
    right_p.wait_recv()
    for p in (1, 2):
        for hc in range(2):
            build(p, hc)
    experts(1, 2)
    combine(2)
    combine(1)
    parts[2].start()
    parts[1].start()
    f_0.wait_recv()
    f_1.wait_recv()
    far_p.start()
    add_part(2)
    add_part(1)

    def piece(ref, h):
        return ref.at[pl.ds(h * half, half), :]

    one_r = remote(piece(mine.at[2], 1), piece(final.at[0], 1), ring_send.at[0], ring_recv.at[0], dev_r)
    one_l = remote(piece(mine.at[1], 0), piece(final.at[1], 0), ring_send.at[1], ring_recv.at[1], dev_l)
    one_r.start()
    one_l.start()
    far_p.wait_recv()
    for hc in range(2):
        build(3, hc)
    experts(3, 1)
    combine(3)
    parts[3].start()
    add_part(3)
    quarter = half // 2
    two, three = [], []
    for k in range(2):
        at_r, at_l, at = pl.ds(k * quarter, quarter), pl.ds(half + k * quarter, quarter), pl.ds(k * quarter, quarter)
        two.append((remote(mine.at[3, at_r, :], relay.at[0, at, :], ring_send.at[2 + k], ring_recv.at[2 + k], dev_r),
                    remote(mine.at[3, at_l, :], relay.at[1, at, :], ring_send.at[4 + k], ring_recv.at[4 + k], dev_l)))
        three.append((remote(mine.at[2, at_r, :], final.at[0, at_r, :], ring_send.at[6 + k], ring_recv.at[6 + k], dev_r),
                      remote(mine.at[1, at_l, :], final.at[1, at_l, :], ring_send.at[8 + k], ring_recv.at[8 + k], dev_l)))
    for pair_of in two:
        for copy in pair_of:
            copy.start()
    add_part(0)

    yb_load.wait()

    def gate_grad(i, carry):
        at = pl.ds(pl.multiple_of(i * 16, 16), 16)
        prod = yb_v[at].astype(F32) * dyall[me, at, :].astype(F32)[:, None, :]
        square[at, 0:top] = jnp.sum(prod, axis=-1)
        return carry
    lax.fori_loop(0, tok // 16, gate_grad, 0)
    dg_ref[...] = square[...].T[0:top, :]

    for k in range(2):
        lo, hi, at = k * quarter, half + k * quarter, slice(k * quarter, (k + 1) * quarter)
        two[k][0].wait_recv()
        mine[2, lo:lo + quarter, :] = mine[2, lo:lo + quarter, :] + relay[0, at, :]
        two[k][1].wait_recv()
        mine[1, hi:hi + quarter, :] = mine[1, hi:hi + quarter, :] + relay[1, at, :]
        three[k][0].start()
        three[k][1].start()
    one_r.wait_recv()
    one_l.wait_recv()
    for k in range(2):
        three[k][0].wait_recv()
        three[k][1].wait_recv()
    dx_ref[...] = (mine[0] + final[0] + final[1]).astype(BF16)

    for copy in metas + [own_p, r_0, l_1, r_1, l_0, f_0, f_1, left_p, right_p, far_p] + parts + [one_r, one_l] + [
            copy for group in two + three for copy in group]:
        copy.wait_send()
    for copy in x_loads:
        copy.wait()


def exchange(ep, dy, topk, slot, gates, y_back, x, h1, h3, w_gate, w_up, w_down):
    tok, width = dy.shape
    n_exp, rows_e, ff = h1.shape
    cap = rows_e // ep
    chips = ep // 2
    top = topk.shape[0]
    any_spec = pl.BlockSpec(memory_space=pl.ANY)
    vmem_spec = pl.BlockSpec(memory_space=pltpu.VMEM)
    dma = pltpu.SemaphoreType.DMA
    return pl.pallas_call(
        functools.partial(exchange_kernel, ep, cap),
        out_shape=(
            jax.ShapeDtypeStruct((tok, width), BF16),
            jax.ShapeDtypeStruct((top, tok), F32),
            pltpu.VMEM((n_exp, rows_e, width), BF16),
            pltpu.VMEM((n_exp, rows_e, width), BF16),
            pltpu.VMEM((n_exp, rows_e, ff), BF16),
            pltpu.VMEM((n_exp, rows_e, ff), BF16),
            pltpu.VMEM((n_exp, rows_e, ff), BF16),
        ),
        in_specs=[any_spec, vmem_spec, vmem_spec, vmem_spec] + [any_spec] * 7,
        out_specs=(vmem_spec,) * 7,
        scratch_shapes=[
            pltpu.VMEM((ep, tok, width), BF16),
            pltpu.VMEM((ep, 2 * top, tok), F32),
            pltpu.VMEM((tok, tok), F32),
            pltpu.VMEM((tok, top, width), BF16),
            pltpu.VMEM((n_exp, rows_e, ff), BF16),
            pltpu.VMEM((n_exp, rows_e, ff), BF16),
            pltpu.VMEM((n_exp, rows_e, ff), F32),
            pltpu.VMEM((n_exp, rows_e, ff), F32),
            pltpu.VMEM((n_exp, width, ff), BF16),
            pltpu.VMEM((n_exp, width, ff), BF16),
            pltpu.VMEM((n_exp, ff, width), BF16),
            pltpu.VMEM((chips, 2, n_exp * cap, tok), BF16),
            pltpu.VMEM((chips, 2, n_exp * cap, width), BF16),
            pltpu.VMEM((chips, tok, width), F32),
            pltpu.VMEM((chips, tok, width), F32),
            pltpu.VMEM((chips, tok, width), F32),
            pltpu.VMEM((2, tok // 2, width), F32),
            pltpu.VMEM((2, tok, width), F32),
            dma((5,)), dma((3, chips)), dma((ep - 1,)), dma((ep - 1,)), dma((6,)), dma((6,)), dma((4,)), dma((4,)),
            dma((chips,)), dma((chips,)), dma((10,)), dma((10,)),
        ],
        compiler_params=pltpu.CompilerParams(collective_id=0, has_side_effects=True, vmem_limit_bytes=46 * 2**20),
        name='exchange',
    )(dy, topk, slot, gates, y_back, x, h1, h3, w_gate, w_up, w_down)


def weight_grad_kernel(x_v, dyd_v, act_v, dh1_v, dh3_v, dwg_hbm, dwu_hbm, dwd_hbm, wide_s, thin_s, sem):
    n_exp, _, width = x_v.shape
    ff = act_v.shape[2]
    hw, hf = width // 2, ff // 2

    def one(e, carry):
        @pl.when(e > 0)
        def _():
            for u in range(6):
                slot(u, e - 1).wait()
        for u in range(2):
            wide_s[u] = dot_tn(act_v[e, :, u * hf:(u + 1) * hf], dyd_v[e])
            slot(u, e).start()
        for u in range(2):
            cols = slice(u * hw, (u + 1) * hw)
            thin_s[u] = dot_tn(x_v[e, :, cols], dh1_v[e])
            slot(2 + u, e).start()
            thin_s[2 + u] = dot_tn(x_v[e, :, cols], dh3_v[e])
            slot(4 + u, e).start()
        return carry

    def slot(u, e):
        if u < 2:
            return pltpu.make_async_copy(wide_s.at[u], dwd_hbm.at[e, pl.ds(u * hf, hf), :], sem.at[u])
        out = dwg_hbm if u < 4 else dwu_hbm
        return pltpu.make_async_copy(thin_s.at[u - 2], out.at[e, pl.ds((u % 2) * hw, hw), :], sem.at[u])

    lax.fori_loop(0, n_exp, one, 0)
    for u in range(6):
        slot(u, n_exp - 1).wait()


def weight_grads(*operands):
    n_exp, _, width = operands[0].shape
    ff = operands[2].shape[2]
    any_spec = pl.BlockSpec(memory_space=pl.ANY)
    vmem_spec = pl.BlockSpec(memory_space=pltpu.VMEM)
    return pl.pallas_call(
        weight_grad_kernel,
        out_shape=(
            jax.ShapeDtypeStruct((n_exp, width, ff), F32),
            jax.ShapeDtypeStruct((n_exp, width, ff), F32),
            jax.ShapeDtypeStruct((n_exp, ff, width), F32),
        ),
        in_specs=[vmem_spec] * 5,
        out_specs=(any_spec,) * 3,
        scratch_shapes=[pltpu.VMEM((2, ff // 2, width), F32), pltpu.VMEM((4, width // 2, ff), F32),
                        pltpu.SemaphoreType.DMA((6,))],
        compiler_params=pltpu.CompilerParams(vmem_limit_bytes=24 * 2**20),
        name='weight_grads',
    )(*[pltpu.with_memory_space_constraint(x, pltpu.VMEM) for x in operands])


def solution(mesh):
    ep = mesh.shape['ep']
    tok_spec = P(('dp', 'ep'), None)
    buf_spec = P(('dp', 'ep'), None, None)
    expert_spec = P('ep', None, None)

    def device_step(dy, topk_idx, slot_idx, gates, y_back, x_disp, h1_disp, h3_disp, w_gate, w_up, w_down):
        dx, d_gates, *saved = exchange(
            ep, dy, topk_idx.T, slot_idx.T, gates.T, y_back, x_disp, h1_disp, h3_disp, w_gate, w_up, w_down)
        dw_gate, dw_up, dw_down = weight_grads(*saved)
        return dx, d_gates.T, dw_gate, dw_up, dw_down

    return jax.shard_map(
        device_step, mesh=mesh,
        in_specs=(tok_spec, tok_spec, tok_spec, tok_spec, buf_spec, buf_spec, buf_spec, buf_spec,
                  expert_spec, expert_spec, expert_spec),
        out_specs=(tok_spec, tok_spec, buf_spec, buf_spec, buf_spec),
        check_vma=False)
```

```python
import functools
import jax
import jax.numpy as jnp
from jax import lax
from jax.experimental import pallas as pl
from jax.experimental.pallas import tpu as pltpu
from jax.sharding import PartitionSpec as P

MESH = pl.DeviceIdType.MESH
F32 = jnp.float32
BF16 = jnp.bfloat16


def dot_nt(a, b):
    return lax.dot_general(a, b, (((1,), (1,)), ((), ())), preferred_element_type=F32)


def dot_tn(a, b):
    return lax.dot_general(a, b, (((0,), (0,)), ((), ())), preferred_element_type=F32)


def exchange_kernel(ep, cap, dy_hbm, topk_hbm, slot_hbm, gate_hbm, yb_hbm, x_hbm, h1_hbm, h3_hbm, wg_hbm, wu_hbm, wd_hbm,
                    dx_ref, dg_ref, xt_v, dyd_v, actt_v, dh_v,
                    dyall, meta, topk_ref, slot_ref, square, yb_v, x_v, h1_v, h3_v, silu_v, slope_v, wg_v, wu_v, wd_v,
                    onehot, dxd, mine, theirs, got, relay, final,
                    load_sem, row_sem, meta_send, meta_recv, dy_send, dy_recv, d2d_send, d2d_recv, part_send, part_recv,
                    ring_send, ring_recv):
    chips = ep // 2
    tok, width = dyall.shape[1], dyall.shape[2]
    half = tok // 2
    n_exp, ff = wd_v.shape[0], wd_v.shape[1]
    top = topk_ref.shape[0]
    pair = 2 * cap
    me = lax.axis_index('ep')
    chip, core = me // 2, me % 2
    right = (chip + 1) % chips
    left = (chip + chips - 1) % chips
    far = (chip + 2) % chips
    dev_r, dev_l, dev_p = right * 2 + core, left * 2 + core, chip * 2 + (1 - core)
    home_f = far * 2 + core
    chip_at = (chip, left, right, far)
    slot_of = (1, 0, 1, 0)

    def remote(src, dst, send_sem, recv_sem, dev):
        return pltpu.make_async_remote_copy(src_ref=src, dst_ref=dst, send_sem=send_sem, recv_sem=recv_sem,
                                            device_id={'ep': dev}, device_id_type=MESH)

    def by_rows(src, dst, i):
        return [pltpu.make_async_copy(src.at[:, pl.ds(chip_at[p] * pair, pair), :],
                                      dst.at[:, pl.ds(p * pair, pair), :], row_sem.at[i, p]) for p in range(chips)]

    own_load = pltpu.make_async_copy(dy_hbm, dyall.at[me], load_sem.at[0])
    h_loads = by_rows(h1_hbm, h1_v, 0) + by_rows(h3_hbm, h3_v, 1)
    w_loads = [pltpu.make_async_copy(src, dst, load_sem.at[i + 1]) for i, (src, dst) in enumerate((
        (wd_hbm, wd_v), (wg_hbm, wg_v), (wu_hbm, wu_v)))]
    yb_load = pltpu.make_async_copy(yb_hbm, yb_v, load_sem.at[4])
    x_loads = by_rows(x_hbm, x_v, 2)
    route_loads = [pltpu.make_async_copy(topk_hbm, topk_ref, load_sem.at[5]),
                   pltpu.make_async_copy(slot_hbm, slot_ref, load_sem.at[6]),
                   pltpu.make_async_copy(gate_hbm, meta.at[me, pl.ds(top, top), :], load_sem.at[7])]

    barrier = pltpu.get_barrier_semaphore()
    for d in range(1, ep):
        pl.semaphore_signal(barrier, inc=1, device_id={'ep': (me + d) % ep}, device_id_type=MESH)
    for copy in [own_load] + route_loads + h_loads + w_loads + x_loads + [yb_load]:
        copy.start()
    square[...] = jnp.zeros_like(square)
    for copy in route_loads:
        copy.wait()
    slot = slot_ref[...]
    meta[me, 0:top, :] = jnp.where(slot >= 0, topk_ref[...] * cap + slot, -1).astype(F32)
    pl.semaphore_wait(barrier, ep - 1)

    own_load.wait()

    def rows(home, h):
        return dyall.at[home, pl.ds(h * half, half), :]

    r_0 = remote(rows(me, 0), rows(me, 0), dy_send.at[0], dy_recv.at[0], dev_r)
    l_1 = remote(rows(me, 1), rows(me, 1), dy_send.at[1], dy_recv.at[1], dev_l)
    r_1 = remote(rows(me, 1), rows(me, 1), dy_send.at[2], dy_recv.at[2], dev_r)
    l_0 = remote(rows(me, 0), rows(me, 0), dy_send.at[3], dy_recv.at[3], dev_l)
    own_p = remote(dyall.at[me], dyall.at[me], d2d_send.at[0], d2d_recv.at[0], dev_p)
    f_0 = remote(rows(dev_l, 0), rows(dev_l, 0), dy_send.at[4], dy_recv.at[4], dev_r)
    f_1 = remote(rows(dev_r, 1), rows(dev_r, 1), dy_send.at[5], dy_recv.at[5], dev_l)
    left_p = remote(dyall.at[dev_l], dyall.at[dev_l], d2d_send.at[1], d2d_recv.at[1], dev_p)
    right_p = remote(dyall.at[dev_r], dyall.at[dev_r], d2d_send.at[2], d2d_recv.at[2], dev_p)
    far_p = remote(dyall.at[home_f], dyall.at[home_f], d2d_send.at[3], d2d_recv.at[3], dev_p)
    m_r, m_l, m_p, m_f, m_lp, m_rp, m_fp = metas = [
        remote(meta.at[home], meta.at[home], meta_send.at[i], meta_recv.at[i], dev) for i, (home, dev) in enumerate((
            (me, dev_r), (me, dev_l), (me, dev_p), (dev_l, dev_r), (dev_l, dev_p), (dev_r, dev_p), (home_f, dev_p)))]
    for copy in (m_r, m_l, r_0, l_1, m_p, own_p, r_1, l_0):
        copy.start()

    def factors(e, carry):
        for p in range(chips):
            span = slice(p * pair, (p + 1) * pair)
            gate_f = h1_v[e, span, :].astype(F32)
            up_f = h3_v[e, span, :].astype(F32)
            sig = jax.nn.sigmoid(gate_f)
            silu = gate_f * sig
            actt_v[e, :, span] = (silu * up_f).astype(BF16).T
            silu_v[e, span, :] = silu
            slope_v[e, span, :] = up_f * sig * (1.0 + gate_f * (1.0 - sig))
        return carry

    def build(p, hc):
        home = chip_at[p] * 2 + hc
        table = meta[home]
        row_id = lax.broadcasted_iota(jnp.int32, (n_exp * cap, tok), 0).astype(F32) + (me * (n_exp * cap)).astype(F32)
        hit = jnp.zeros((n_exp * cap, tok), F32)
        gate = jnp.zeros((n_exp * cap, tok), F32)
        for j in range(top):
            same = row_id == table[j:j + 1, :]
            hit = jnp.where(same, 1.0, hit)
            gate = jnp.where(same, table[top + j:top + j + 1, :], gate)
        gate_row = jnp.sum(gate, axis=1, keepdims=True)
        sel = hit.astype(BF16)
        onehot[p, hc] = sel
        at = pl.ds(pl.multiple_of(p * pair + hc * cap, cap), cap)
        for n in range(width // 256):
            cols = slice(n * 256, (n + 1) * 256)
            block = (jnp.dot(sel, dyall[home, :, cols], preferred_element_type=F32) * gate_row).astype(BF16)
            for e in range(n_exp):
                dyd_v[e, at, cols] = block[e * cap:(e + 1) * cap]

    def experts(p, count):
        span = slice(p * pair, (p + count) * pair)
        for e in range(n_exp):
            d_act = dot_nt(dyd_v[e, span, :], wd_v[e]).astype(BF16).astype(F32)
            dh1 = (d_act * slope_v[e, span, :]).astype(BF16)
            dh3 = (d_act * silu_v[e, span, :]).astype(BF16)
            dh_v[e, span, 0:ff] = dh1
            dh_v[e, span, ff:2 * ff] = dh3
            out = (dot_nt(dh1, wg_v[e]) + dot_nt(dh3, wu_v[e])).astype(BF16)
            for q in range(2 * count):
                dxd[slot_of[p + q // 2], q % 2, e * cap:(e + 1) * cap, :] = out[q * cap:(q + 1) * cap]

    def sum_theirs(p):
        theirs[p] = dot_tn(onehot[p, 1 - core], dxd[slot_of[p], 1 - core])

    def sum_mine(p):
        mine[p] = dot_tn(onehot[p, core], dxd[slot_of[p], core])

    parts = [remote(theirs.at[p], got.at[p], part_send.at[p], part_recv.at[p], dev_p) for p in range(chips)]
    first, last = slice(0, half), slice(half, tok)

    def add_part(p, at):
        mine[p, at, :] = mine[p, at, :] + got[p, at, :]

    def piece(ref, h):
        return ref.at[pl.ds(h * half, half), :]

    one_r = remote(piece(mine.at[2], 1), piece(final.at[0], 1), ring_send.at[0], ring_recv.at[0], dev_r)
    one_l = remote(piece(mine.at[1], 0), piece(final.at[1], 0), ring_send.at[1], ring_recv.at[1], dev_l)
    quarter = half // 2
    two, three = [], []
    for k in range(2):
        at_r, at_l, at = pl.ds(k * quarter, quarter), pl.ds(half + k * quarter, quarter), pl.ds(k * quarter, quarter)
        two.append((remote(mine.at[3, at_r, :], relay.at[0, at, :], ring_send.at[2 + k], ring_recv.at[2 + k], dev_r),
                    remote(mine.at[3, at_l, :], relay.at[1, at, :], ring_send.at[4 + k], ring_recv.at[4 + k], dev_l)))
        three.append((remote(mine.at[2, at_r, :], final.at[0, at_r, :], ring_send.at[6 + k], ring_recv.at[6 + k], dev_r),
                      remote(mine.at[1, at_l, :], final.at[1, at_l, :], ring_send.at[8 + k], ring_recv.at[8 + k], dev_l)))

    for copy in h_loads:
        copy.wait()
    m_r.wait_recv()
    m_f.start()
    lax.fori_loop(0, n_exp, factors, 0)
    r_0.wait_recv()
    f_0.start()
    l_1.wait_recv()
    f_1.start()
    m_lp.start()
    m_l.wait_recv()
    m_rp.start()
    r_1.wait_recv()
    left_p.start()
    l_0.wait_recv()
    right_p.start()
    build(1, core)
    build(2, core)
    m_lp.wait_recv()
    left_p.wait_recv()
    build(1, 1 - core)
    m_rp.wait_recv()
    right_p.wait_recv()
    build(2, 1 - core)
    for copy in w_loads:
        copy.wait()
    experts(1, 2)
    sum_theirs(2)
    sum_theirs(1)
    sum_mine(2)
    parts[2].start()
    parts[1].start()
    sum_mine(1)
    m_f.wait_recv()
    m_fp.start()
    f_0.wait_recv()
    f_1.wait_recv()
    far_p.start()
    parts[2].wait_recv()
    add_part(2, last)
    parts[1].wait_recv()
    add_part(1, first)
    one_r.start()
    one_l.start()
    add_part(2, first)
    add_part(1, last)
    build(3, core)
    m_fp.wait_recv()
    far_p.wait_recv()
    build(3, 1 - core)
    experts(3, 1)
    sum_theirs(3)
    sum_mine(3)
    parts[3].start()
    m_p.wait_recv()
    own_p.wait_recv()
    build(0, core)
    build(0, 1 - core)
    parts[3].wait_recv()
    add_part(3, first)
    add_part(3, last)
    for group in two:
        for copy in group:
            copy.start()
    experts(0, 1)
    sum_theirs(0)
    sum_mine(0)
    parts[0].start()

    yb_load.wait()

    def gate_grad(i, carry):
        at = pl.ds(pl.multiple_of(i * 16, 16), 16)
        prod = yb_v[at].astype(F32) * dyall[me, at, :].astype(F32)[:, None, :]
        square[at, 0:top] = jnp.sum(prod, axis=-1)
        return carry
    lax.fori_loop(0, tok // 16, gate_grad, 0)
    dg_ref[...] = square[...].T[0:top, :]
    parts[0].wait_recv()
    add_part(0, first)
    add_part(0, last)

    for k in range(2):
        lo, hi, at = k * quarter, half + k * quarter, slice(k * quarter, (k + 1) * quarter)
        two[k][0].wait_recv()
        mine[2, lo:lo + quarter, :] = mine[2, lo:lo + quarter, :] + relay[0, at, :]
        two[k][1].wait_recv()
        mine[1, hi:hi + quarter, :] = mine[1, hi:hi + quarter, :] + relay[1, at, :]
        three[k][0].start()
        three[k][1].start()
    for copy in x_loads:
        copy.wait()

    def turn(e, carry):
        for p in range(chips):
            span = slice(p * pair, (p + 1) * pair)
            xt_v[e, :, span] = x_v[e, span, :].T
        return carry
    lax.fori_loop(0, n_exp, turn, 0)
    one_r.wait_recv()
    one_l.wait_recv()
    for k in range(2):
        three[k][0].wait_recv()
        three[k][1].wait_recv()
    dx_ref[...] = (mine[0] + final[0] + final[1]).astype(BF16)

    for copy in metas + [own_p, r_0, l_1, r_1, l_0, f_0, f_1, left_p, right_p, far_p] + parts + [one_r, one_l] + [
            copy for group in two + three for copy in group]:
        copy.wait_send()


def exchange(ep, dy, topk, slot, gates, y_back, x, h1, h3, w_gate, w_up, w_down):
    tok, width = dy.shape
    n_exp, rows_e, ff = h1.shape
    cap = rows_e // ep
    chips = ep // 2
    top = topk.shape[0]
    any_spec = pl.BlockSpec(memory_space=pl.ANY)
    vmem_spec = pl.BlockSpec(memory_space=pltpu.VMEM)
    dma = pltpu.SemaphoreType.DMA
    return pl.pallas_call(
        functools.partial(exchange_kernel, ep, cap),
        out_shape=(
            pltpu.VMEM((tok, width), BF16),
            pltpu.VMEM((top, tok), F32),
            pltpu.VMEM((n_exp, width, rows_e), BF16),
            pltpu.VMEM((n_exp, rows_e, width), BF16),
            pltpu.VMEM((n_exp, ff, rows_e), BF16),
            pltpu.VMEM((n_exp, rows_e, 2 * ff), BF16),
        ),
        in_specs=[any_spec] * 11,
        out_specs=(vmem_spec,) * 6,
        scratch_shapes=[
            pltpu.VMEM((ep, tok, width), BF16),
            pltpu.VMEM((ep, 2 * top, tok), F32),
            pltpu.VMEM((top, tok), jnp.int32),
            pltpu.VMEM((top, tok), jnp.int32),
            pltpu.VMEM((tok, tok), F32),
            pltpu.VMEM((tok, top, width), BF16),
            pltpu.VMEM((n_exp, rows_e, width), BF16),
            pltpu.VMEM((n_exp, rows_e, ff), BF16),
            pltpu.VMEM((n_exp, rows_e, ff), BF16),
            pltpu.VMEM((n_exp, rows_e, ff), F32),
            pltpu.VMEM((n_exp, rows_e, ff), F32),
            pltpu.VMEM((n_exp, width, ff), BF16),
            pltpu.VMEM((n_exp, width, ff), BF16),
            pltpu.VMEM((n_exp, ff, width), BF16),
            pltpu.VMEM((chips, 2, n_exp * cap, tok), BF16),
            pltpu.VMEM((2, 2, n_exp * cap, width), BF16),
            pltpu.VMEM((chips, tok, width), F32),
            pltpu.VMEM((chips, tok, width), F32),
            pltpu.VMEM((chips, tok, width), F32),
            pltpu.VMEM((2, tok // 2, width), F32),
            pltpu.VMEM((2, tok, width), F32),
            dma((8,)), dma((3, chips)), dma((7,)), dma((7,)), dma((6,)), dma((6,)), dma((4,)), dma((4,)),
            dma((chips,)), dma((chips,)), dma((10,)), dma((10,)),
        ],
        compiler_params=pltpu.CompilerParams(collective_id=0, has_side_effects=True, vmem_limit_bytes=44 * 2**20),
        name='exchange',
    )(dy, topk, slot, gates, y_back, x, h1, h3, w_gate, w_up, w_down)


def weight_grad_kernel(dx_v, dg_v, xt_v, dyd_v, actt_v, dh_v, dx_hbm, dg_hbm, dwg_hbm, dwu_hbm, dwd_hbm, stage, sem, small_sem):
    n_exp, width, _ = xt_v.shape
    ff = actt_v.shape[1]
    block = stage.shape[1]
    down = ff // block
    small = [pltpu.make_async_copy(dx_v, dx_hbm, small_sem.at[0]), pltpu.make_async_copy(dg_v, dg_hbm, small_sem.at[1])]

    def copies(u, e):
        if u < down:
            return [pltpu.make_async_copy(stage.at[u], dwd_hbm.at[e, pl.ds(u * block, block), :], sem.at[u, 0])]
        at = pl.ds((u - down) * block, block)
        return [pltpu.make_async_copy(stage.at[u, :, pl.ds(0, ff)], dwg_hbm.at[e, at, :], sem.at[u, 0]),
                pltpu.make_async_copy(stage.at[u, :, pl.ds(ff, ff)], dwu_hbm.at[e, at, :], sem.at[u, 1])]

    def one(e, carry):
        for u in range(stage.shape[0]):
            @pl.when(e > 0)
            def _():
                for copy in copies(u, e - 1):
                    copy.wait()
            if u < down:
                stage[u] = jnp.dot(actt_v[e, u * block:(u + 1) * block, :], dyd_v[e], preferred_element_type=F32)
            else:
                at = slice((u - down) * block, (u - down + 1) * block)
                stage[u] = jnp.dot(xt_v[e, at, :], dh_v[e], preferred_element_type=F32)
            for copy in copies(u, e):
                copy.start()
        return carry

    for copy in small:
        copy.start()
    lax.fori_loop(0, n_exp, one, 0)
    for u in range(stage.shape[0]):
        for copy in copies(u, n_exp - 1):
            copy.wait()
    for copy in small:
        copy.wait()


def weight_grads(dx, d_gates, xt, dyd, actt, dh):
    n_exp, width, _ = xt.shape
    ff = actt.shape[1]
    block = 256
    units = (width + ff) // block
    any_spec = pl.BlockSpec(memory_space=pl.ANY)
    vmem_spec = pl.BlockSpec(memory_space=pltpu.VMEM)
    return pl.pallas_call(
        weight_grad_kernel,
        out_shape=(
            jax.ShapeDtypeStruct(dx.shape, dx.dtype),
            jax.ShapeDtypeStruct(d_gates.shape, d_gates.dtype),
            jax.ShapeDtypeStruct((n_exp, width, ff), F32),
            jax.ShapeDtypeStruct((n_exp, width, ff), F32),
            jax.ShapeDtypeStruct((n_exp, ff, width), F32),
        ),
        in_specs=[vmem_spec] * 6,
        out_specs=(any_spec,) * 5,
        scratch_shapes=[pltpu.VMEM((units, block, width), F32), pltpu.SemaphoreType.DMA((units, 2)),
                        pltpu.SemaphoreType.DMA((2,))],
        compiler_params=pltpu.CompilerParams(vmem_limit_bytes=16 * 2**20),
        name='weight_grads',
    )(*[pltpu.with_memory_space_constraint(x, pltpu.VMEM) for x in (dx, d_gates, xt, dyd, actt, dh)])


def solution(mesh):
    ep = mesh.shape['ep']
    tok_spec = P(('dp', 'ep'), None)
    buf_spec = P(('dp', 'ep'), None, None)
    expert_spec = P('ep', None, None)

    def device_step(dy, topk_idx, slot_idx, gates, y_back, x_disp, h1_disp, h3_disp, w_gate, w_up, w_down):
        saved = exchange(
            ep, dy, topk_idx.T, slot_idx.T, gates.T, y_back, x_disp, h1_disp, h3_disp, w_gate, w_up, w_down)
        dx, d_gates, dw_gate, dw_up, dw_down = weight_grads(*saved)
        return dx, d_gates.T, dw_gate, dw_up, dw_down

    return jax.shard_map(
        device_step, mesh=mesh,
        in_specs=(tok_spec, tok_spec, tok_spec, tok_spec, buf_spec, buf_spec, buf_spec, buf_spec,
                  expert_spec, expert_spec, expert_spec),
        out_specs=(tok_spec, tok_spec, buf_spec, buf_spec, buf_spec),
        check_vma=False)
```

```python
import functools
import jax
import jax.numpy as jnp
from jax import lax
from jax.experimental import pallas as pl
from jax.experimental.pallas import tpu as pltpu
from jax.sharding import PartitionSpec as P

MESH = pl.DeviceIdType.MESH
F32 = jnp.float32
BF16 = jnp.bfloat16


def dot_tn(a, b):
    return lax.dot_general(a, b, (((0,), (0,)), ((), ())), preferred_element_type=F32)


def exchange_kernel(ep, cap, dy_hbm, topk_hbm, slot_hbm, gate_hbm, yb_hbm, x_hbm, h1_hbm, h3_hbm, wg_hbm, wu_hbm, wd_hbm,
                    dx_ref, dg_ref, xt_v, dyd_v, actt_v, dh_v,
                    dyall, meta, topk_v, slot_v, square, yb_v, x_v, h1_v, h3_v, silu_v, slope_v, wgt_v, wut_v, wdt_v,
                    onehot, dxd, mine, theirs, got, fsum, fgot, own, relay, final,
                    load_sem, row_sem, meta_send, meta_recv, dy_send, dy_recv, d2d_send, d2d_recv, part_send, part_recv,
                    ring_send, ring_recv):
    chips = ep // 2
    tok, width = dyall.shape[1], dyall.shape[2]
    half = tok // 2
    n_exp, ff = wgt_v.shape[0], wgt_v.shape[1]
    top = topk_v.shape[0]
    pair = 2 * cap
    me = lax.axis_index('ep')
    chip, core = me // 2, me % 2
    right = (chip + 1) % chips
    left = (chip + chips - 1) % chips
    far = (chip + 2) % chips
    dev_r, dev_l, dev_p = right * 2 + core, left * 2 + core, chip * 2 + (1 - core)
    ahead = right * (1 - core) + left * core
    behind = left * (1 - core) + right * core
    dev_a = ahead * 2 + core
    home_of = (left * 2, right * 2, left * 2 + 1, right * 2 + 1, far * 2, far * 2 + 1, chip * 2, chip * 2 + 1)

    def remote(src, dst, send_sem, recv_sem, dev):
        return pltpu.make_async_remote_copy(src_ref=src, dst_ref=dst, send_sem=send_sem, recv_sem=recv_sem,
                                            device_id={'ep': dev}, device_id_type=MESH)

    def load(src, dst, i):
        return pltpu.make_async_copy(src, dst, load_sem.at[i])

    def by_rows(src, dst, i):
        return [pltpu.make_async_copy(src.at[:, pl.ds(pl.multiple_of(home_of[b] * cap, cap), cap), :],
                                      dst.at[:, pl.ds(b * cap, cap), :], row_sem.at[i, b]) for b in range(ep)]

    own_load = load(dy_hbm, dyall.at[me], 0)
    route_loads = [load(topk_hbm, topk_v, 1), load(slot_hbm, slot_v, 2),
                   load(gate_hbm, meta.at[me, pl.ds(top, top), :], 3)]
    h_loads = by_rows(h1_hbm, h1_v, 0) + by_rows(h3_hbm, h3_v, 1)
    wd_load, wg_load = load(wd_hbm, dyd_v, 4), load(wg_hbm, xt_v, 5)
    wu_loads = [load(wu_hbm.at[:, pl.ds(i * ff, ff), :], x_v.at[:, :, pl.ds(i * ff, ff)], 6 + i) for i in range(2)]
    yb_load = load(yb_hbm, yb_v, 8)
    x_loads = by_rows(x_hbm, x_v, 2)

    barrier = pltpu.get_barrier_semaphore()
    for d in range(1, ep):
        pl.semaphore_signal(barrier, inc=1, device_id={'ep': (me + d) % ep}, device_id_type=MESH)
    for copy in [own_load] + route_loads + h_loads + [wd_load, wg_load] + wu_loads + [yb_load]:
        copy.start()
    square[...] = jnp.zeros_like(square)
    for copy in route_loads:
        copy.wait()
    slot = slot_v[...]
    meta[me, 0:top, :] = jnp.where(slot >= 0, topk_v[...] * cap + slot, -1).astype(F32)
    own_load.wait()
    pl.semaphore_wait(barrier, ep - 1)

    def rows(ref, home, h):
        return ref.at[home, pl.ds(pl.multiple_of(h * half, half), half), :]

    def dy_copy(home, h, send_sem, recv_sem, dev):
        return remote(rows(dyall, home, h), rows(dyall, home, h), send_sem, recv_sem, dev)

    own_a = dy_copy(me, 1 - core, d2d_send.at[0], d2d_recv.at[0], dev_p)
    own_b = dy_copy(me, core, d2d_send.at[1], d2d_recv.at[1], dev_p)
    to_r = [dy_copy(chip * 2 + q, core, dy_send.at[q], dy_recv.at[q], dev_r) for q in range(2)]
    to_l = [dy_copy(chip * 2 + q, core, dy_send.at[2 + q], dy_recv.at[2 + q], dev_l) for q in range(2)]
    hop = [dy_copy(behind * 2 + q, core, dy_send.at[4 + q], dy_recv.at[4 + q], dev_a) for q in range(2)]
    left_p = [dy_copy(left * 2 + q, core, d2d_send.at[2 + q], d2d_recv.at[2 + q], dev_p) for q in range(2)]
    right_p = [dy_copy(right * 2 + q, core, d2d_send.at[4 + q], d2d_recv.at[4 + q], dev_p) for q in range(2)]
    far_p = [dy_copy(far * 2 + q, core, d2d_send.at[6 + q], d2d_recv.at[6 + q], dev_p) for q in range(2)]
    m_r, m_l, m_p, m_f, m_lp, m_rp, m_fp = metas = [
        remote(meta.at[home], meta.at[home], meta_send.at[i], meta_recv.at[i], dev) for i, (home, dev) in enumerate((
            (me, dev_r), (me, dev_l), (me, dev_p), (dev_l, dev_r), (dev_l, dev_p), (dev_r, dev_p), (far * 2 + core, dev_p)))]

    def start_first():
        to_r[0].start()
        to_l[0].start()

    own_a.start()
    pl.when(core == 0)(start_first)
    for copy in (m_r, m_l, m_p, own_b):
        copy.start()

    def factors(e, carry):
        for p in range(chips):
            span = slice(p * pair, (p + 1) * pair)
            gate_f = h1_v[e, span, :].astype(F32)
            up_f = h3_v[e, span, :].astype(F32)
            sig = jax.nn.sigmoid(gate_f)
            silu = gate_f * sig
            actt_v[e, :, span] = (silu * up_f).astype(BF16).T
            silu_v[e, span, :] = silu
            slope_v[e, span, :] = up_f * sig * (1.0 + gate_f * (1.0 - sig))
        return carry

    def build(b):
        home = home_of[b]
        table = meta[home]
        row_id = lax.broadcasted_iota(jnp.int32, (n_exp * cap, tok), 0).astype(F32) + (me * (n_exp * cap)).astype(F32)
        hit = jnp.zeros((n_exp * cap, tok), F32)
        gate = jnp.zeros((n_exp * cap, tok), F32)
        for j in range(top):
            same = row_id == table[j:j + 1, :]
            hit = jnp.where(same, 1.0, hit)
            gate = jnp.where(same, table[top + j:top + j + 1, :], gate)
        gate_row = jnp.sum(gate, axis=1, keepdims=True)
        sel = hit.astype(BF16)
        onehot[b] = sel
        for n in range(width // 256):
            cols = slice(n * 256, (n + 1) * 256)
            block = (jnp.dot(sel, dyall[home, :, cols], preferred_element_type=F32) * gate_row).astype(BF16)
            for e in range(n_exp):
                dyd_v[e, b * cap:(b + 1) * cap, cols] = block[e * cap:(e + 1) * cap]

    def experts(k, between):
        span = slice(k * pair, (k + 1) * pair)
        for e in range(n_exp):
            d_act = jnp.dot(dyd_v[e, span, :], wdt_v[e], preferred_element_type=F32).astype(BF16).astype(F32)
            dh_v[e, span, 0:ff] = (d_act * slope_v[e, span, :]).astype(BF16)
            dh_v[e, span, ff:2 * ff] = (d_act * silu_v[e, span, :]).astype(BF16)
        between()
        for e in range(n_exp):
            out = (jnp.dot(dh_v[e, span, 0:ff], wgt_v[e], preferred_element_type=F32)
                   + jnp.dot(dh_v[e, span, ff:2 * ff], wut_v[e], preferred_element_type=F32)).astype(BF16)
            for j in range(2):
                dxd[k % 2, j, e * cap:(e + 1) * cap, :] = out[j * cap:(j + 1) * cap]

    def token_sum(k, j):
        return dot_tn(onehot[2 * k + j], dxd[k % 2, j])

    def piece(h):
        return pl.ds(pl.multiple_of(h * half, half), half)

    part_a = [remote(theirs.at[q, piece(core), :], got.at[q, piece(core), :], part_send.at[q], part_recv.at[q], dev_p)
              for q in range(2)]
    part_b = [remote(theirs.at[q, piece(1 - core), :], got.at[q, piece(1 - core), :], part_send.at[2 + q],
                     part_recv.at[2 + q], dev_p) for q in range(2)]
    part_f = [remote(fsum.at[q, piece(1 - core), :], fgot.at[q], part_send.at[4 + q], part_recv.at[4 + q], dev_p)
              for q in range(2)]
    part_o = remote(own.at[1], own.at[2], part_send.at[6], part_recv.at[6], dev_p)
    one = [remote(mine.at[q, piece(1 - core), :], final.at[core, piece(1 - core), :], ring_send.at[q], ring_recv.at[core],
                  ahead * 2 + q) for q in range(2)]
    two = [remote(fsum.at[q, piece(core), :], relay.at[q], ring_send.at[2 + q], ring_recv.at[2 + q], dev_a)
           for q in range(2)]
    three = [remote(mine.at[q, piece(core), :], final.at[core, piece(core), :], ring_send.at[4 + q],
                    ring_recv.at[4 + core], ahead * 2 + q) for q in range(2)]

    def landed(direction, h, sem):
        where = final.at[direction, pl.ds(h * half, half), :]
        remote(where, where, ring_send.at[0], ring_recv.at[sem], dev_p).wait_recv()

    def next_homes():
        to_r[1].wait_recv()
        left_p[1].start()
        to_l[1].wait_recv()
        right_p[1].start()
        hop[1].start()

    def send_one(q):
        part_a[q].wait_recv()
        at = piece(1 - core)
        mine[q, at, :] = mine[q, at, :] + got[q, at, :]
        one[q].start()

    def sums(q):
        theirs[q] = token_sum(q, core)
        mine[q] = token_sum(q, 1 - core)
        part_a[q].start()
        part_b[q].start()

    for copy in h_loads:
        copy.wait()
    own_a.wait_recv()
    pl.when(core == 1)(start_first)
    to_r[1].start()
    to_l[1].start()
    lax.fori_loop(0, n_exp, factors, 0)
    m_r.wait_recv()
    m_f.start()
    m_lp.start()
    m_l.wait_recv()
    m_rp.start()

    def turn_down(e, carry):
        wdt_v[e] = dyd_v[e].T
        return carry

    def turn_gate(e, carry):
        wgt_v[e] = xt_v[e].T
        return carry

    def turn_up(e, carry):
        for i in range(2):
            wut_v[e, :, i * ff:(i + 1) * ff] = x_v[e, :, i * ff:(i + 1) * ff].T
        return carry

    wd_load.wait()
    lax.fori_loop(0, n_exp, turn_down, 0)
    wg_load.wait()
    lax.fori_loop(0, n_exp, turn_gate, 0)
    for copy in wu_loads:
        copy.wait()
    lax.fori_loop(0, n_exp, turn_up, 0)
    for copy in x_loads:
        copy.start()

    to_r[0].wait_recv()
    left_p[0].start()
    to_l[0].wait_recv()
    right_p[0].start()
    hop[0].start()
    m_lp.wait_recv()
    m_rp.wait_recv()
    left_p[0].wait_recv()
    build(0)
    right_p[0].wait_recv()
    build(1)
    experts(0, next_homes)
    sums(0)
    left_p[1].wait_recv()
    build(2)
    right_p[1].wait_recv()
    build(3)

    def far_homes():
        send_one(0)
        m_f.wait_recv()
        m_fp.start()
        for q in range(2):
            hop[q].wait_recv()
            far_p[q].start()

    experts(1, far_homes)
    sums(1)
    m_fp.wait_recv()
    for q in range(2):
        far_p[q].wait_recv()
        build(4 + q)
    experts(2, lambda: send_one(1))
    for q in range(2):
        fsum[q] = token_sum(2, q)
    for q in range(2):
        part_f[q].start()
    m_p.wait_recv()
    own_b.wait_recv()
    build(6)
    build(7)

    def send_two():
        for q in range(2):
            part_f[q].wait_recv()
            at = piece(core)
            fsum[q, at, :] = fsum[q, at, :] + fgot[q]
            two[q].start()

    send_two()
    experts(3, lambda: None)
    own[1] = token_sum(3, 1 - core)
    own[0] = token_sum(3, core)
    part_o.start()
    for q in range(2):
        part_b[q].wait_recv()
        at = piece(core)
        mine[q, at, :] = mine[q, at, :] + got[q, at, :]

    yb_load.wait()

    def gate_grad(i, carry):
        at = pl.ds(pl.multiple_of(i * 16, 16), 16)
        prod = yb_v[at].astype(F32) * dyall[me, at, :].astype(F32)[:, None, :]
        square[at, 0:top] = jnp.sum(prod, axis=-1)
        return carry
    lax.fori_loop(0, tok // 16, gate_grad, 0)
    dg_ref[...] = square[...].T[0:top, :]
    part_o.wait_recv()
    own[0] = own[0] + own[2]

    for q in range(2):
        two[q].wait_recv()
        at = piece(core)
        mine[q, at, :] = mine[q, at, :] + relay[q]
        three[q].start()
    for copy in x_loads:
        copy.wait()

    def turn(e, carry):
        for p in range(chips):
            span = slice(p * pair, (p + 1) * pair)
            xt_v[e, :, span] = x_v[e, span, :].T
        return carry
    lax.fori_loop(0, n_exp, turn, 0)
    landed(0, 1, 0)
    landed(1, 0, 1)
    landed(0, 0, 4)
    landed(1, 1, 5)
    dx_ref[...] = (own[0] + final[0] + final[1]).astype(BF16)

    for copy in metas + [own_a, own_b] + to_r + to_l + hop + left_p + right_p + far_p + part_a + part_b + part_f + [
            part_o] + one + two + three:
        copy.wait_send()


def exchange(ep, dy, topk, slot, gates, y_back, x, h1, h3, w_gate, w_up, w_down):
    tok, width = dy.shape
    n_exp, rows_e, ff = h1.shape
    cap = rows_e // ep
    top = topk.shape[0]
    any_spec = pl.BlockSpec(memory_space=pl.ANY)
    vmem_spec = pl.BlockSpec(memory_space=pltpu.VMEM)
    dma = pltpu.SemaphoreType.DMA
    return pl.pallas_call(
        functools.partial(exchange_kernel, ep, cap),
        out_shape=(
            pltpu.VMEM((tok, width), BF16),
            pltpu.VMEM((top, tok), F32),
            pltpu.VMEM((n_exp, width, rows_e), BF16),
            pltpu.VMEM((n_exp, rows_e, width), BF16),
            pltpu.VMEM((n_exp, ff, rows_e), BF16),
            pltpu.VMEM((n_exp, rows_e, 2 * ff), BF16),
        ),
        in_specs=[any_spec] * 11,
        out_specs=(vmem_spec,) * 6,
        scratch_shapes=[
            pltpu.VMEM((ep, tok, width), BF16),
            pltpu.VMEM((ep, 2 * top, tok), F32),
            pltpu.VMEM((top, tok), jnp.int32),
            pltpu.VMEM((top, tok), jnp.int32),
            pltpu.VMEM((tok, tok), F32),
            pltpu.VMEM((tok, top, width), BF16),
            pltpu.VMEM((n_exp, rows_e, width), BF16),
            pltpu.VMEM((n_exp, rows_e, ff), BF16),
            pltpu.VMEM((n_exp, rows_e, ff), BF16),
            pltpu.VMEM((n_exp, rows_e, ff), F32),
            pltpu.VMEM((n_exp, rows_e, ff), F32),
            pltpu.VMEM((n_exp, ff, width), BF16),
            pltpu.VMEM((n_exp, ff, width), BF16),
            pltpu.VMEM((n_exp, width, ff), BF16),
            pltpu.VMEM((ep, n_exp * cap, tok), BF16),
            pltpu.VMEM((2, 2, n_exp * cap, width), BF16),
            pltpu.VMEM((2, tok, width), F32),
            pltpu.VMEM((2, tok, width), F32),
            pltpu.VMEM((2, tok, width), F32),
            pltpu.VMEM((2, tok, width), F32),
            pltpu.VMEM((2, tok // 2, width), F32),
            pltpu.VMEM((3, tok, width), F32),
            pltpu.VMEM((2, tok // 2, width), F32),
            pltpu.VMEM((2, tok, width), F32),
            dma((9,)), dma((3, ep)), dma((7,)), dma((7,)), dma((6,)), dma((6,)), dma((8,)), dma((8,)),
            dma((7,)), dma((7,)), dma((6,)), dma((6,)),
        ],
        compiler_params=pltpu.CompilerParams(collective_id=0, has_side_effects=True, vmem_limit_bytes=44 * 2**20),
        name='exchange',
    )(dy, topk, slot, gates, y_back, x, h1, h3, w_gate, w_up, w_down)


def weight_grad_kernel(dx_v, dg_v, xt_v, dyd_v, actt_v, dh_v, dx_hbm, dg_hbm, dwg_hbm, dwu_hbm, dwd_hbm, stage, sem, small_sem):
    n_exp, width, _ = xt_v.shape
    ff = actt_v.shape[1]
    slots, block = stage.shape[0], stage.shape[1]
    down = ff // block
    units = [(u, e) for e in range(n_exp) for u in range((ff + width) // block)]
    small = [pltpu.make_async_copy(dx_v, dx_hbm, small_sem.at[0]), pltpu.make_async_copy(dg_v, dg_hbm, small_sem.at[1])]
    for copy in small:
        copy.start()

    def copies(i):
        (u, e), s = units[i], i % slots
        if u < down:
            return [pltpu.make_async_copy(stage.at[s], dwd_hbm.at[e, pl.ds(u * block, block), :], sem.at[s, 0])]
        at = pl.ds((u - down) * block, block)
        return [pltpu.make_async_copy(stage.at[s, :, pl.ds(0, ff)], dwg_hbm.at[e, at, :], sem.at[s, 0]),
                pltpu.make_async_copy(stage.at[s, :, pl.ds(ff, ff)], dwu_hbm.at[e, at, :], sem.at[s, 1])]

    for i, (u, e) in enumerate(units):
        if i >= slots:
            for copy in copies(i - slots):
                copy.wait()
        if u < down:
            stage[i % slots] = jnp.dot(actt_v[e, u * block:(u + 1) * block, :], dyd_v[e], preferred_element_type=F32)
        else:
            at = slice((u - down) * block, (u - down + 1) * block)
            stage[i % slots] = jnp.dot(xt_v[e, at, :], dh_v[e], preferred_element_type=F32)
        for copy in copies(i):
            copy.start()
    for i in range(len(units) - slots, len(units)):
        for copy in copies(i):
            copy.wait()
    for copy in small:
        copy.wait()


def weight_grads(dx, d_gates, xt, dyd, actt, dh):
    n_exp, width, _ = xt.shape
    ff = actt.shape[1]
    block, slots = 512, 4
    any_spec = pl.BlockSpec(memory_space=pl.ANY)
    vmem_spec = pl.BlockSpec(memory_space=pltpu.VMEM)
    return pl.pallas_call(
        weight_grad_kernel,
        out_shape=(
            jax.ShapeDtypeStruct(dx.shape, dx.dtype),
            jax.ShapeDtypeStruct(d_gates.shape, d_gates.dtype),
            jax.ShapeDtypeStruct((n_exp, width, ff), F32),
            jax.ShapeDtypeStruct((n_exp, width, ff), F32),
            jax.ShapeDtypeStruct((n_exp, ff, width), F32),
        ),
        in_specs=[vmem_spec] * 6,
        out_specs=(any_spec,) * 5,
        scratch_shapes=[pltpu.VMEM((slots, block, width), F32), pltpu.SemaphoreType.DMA((slots, 2)),
                        pltpu.SemaphoreType.DMA((2,))],
        compiler_params=pltpu.CompilerParams(vmem_limit_bytes=20 * 2**20),
        cost_estimate=pl.CostEstimate(flops=6 * n_exp * xt.shape[2] * width * ff, transcendentals=0,
                                      bytes_accessed=12 * n_exp * width * ff),
        name='weight_grads',
    )(*[pltpu.with_memory_space_constraint(x, pltpu.VMEM) for x in (dx, d_gates, xt, dyd, actt, dh)])


def solution(mesh):
    ep = mesh.shape['ep']
    tok_spec = P(('dp', 'ep'), None)
    buf_spec = P(('dp', 'ep'), None, None)
    expert_spec = P('ep', None, None)

    def device_step(dy, topk_idx, slot_idx, gates, y_back, x_disp, h1_disp, h3_disp, w_gate, w_up, w_down):
        saved = exchange(
            ep, dy, topk_idx.T, slot_idx.T, gates.T, y_back, x_disp, h1_disp, h3_disp, w_gate, w_up, w_down)
        dx, d_gates, dw_gate, dw_up, dw_down = weight_grads(*saved)
        return dx, d_gates.T, dw_gate, dw_up, dw_down

    return jax.shard_map(
        device_step, mesh=mesh,
        in_specs=(tok_spec, tok_spec, tok_spec, tok_spec, buf_spec, buf_spec, buf_spec, buf_spec,
                  expert_spec, expert_spec, expert_spec),
        out_specs=(tok_spec, tok_spec, buf_spec, buf_spec, buf_spec),
        check_vma=False)
```

```python
import functools
import jax
import jax.numpy as jnp
from jax import lax
from jax.experimental import pallas as pl
from jax.experimental.pallas import tpu as pltpu
from jax.sharding import PartitionSpec as P

MESH = pl.DeviceIdType.MESH
F32 = jnp.float32
BF16 = jnp.bfloat16


def dot_tn(a, b):
    return lax.dot_general(a, b, (((0,), (0,)), ((), ())), preferred_element_type=F32)


def exchange_kernel(ep, cap, dy_hbm, topk_hbm, slot_hbm, gate_hbm, yb_hbm, x_hbm, h1_hbm, h3_hbm, wg_hbm, wu_hbm, wd_hbm,
                    dx_ref, dg_ref, first_ref, xt_v, dyd_v, actt_v, dh_v,
                    dyall, meta, topk_v, slot_v, square, yb_v, x_v, h1_v, h3_v, silu_v, slope_v, wgt_v, wut_v, wdt_v,
                    onehot, dxd, mine, theirs, got, fsum, fgot, own, relay, final,
                    load_sem, row_sem, meta_send, meta_recv, dy_send, dy_recv, d2d_send, d2d_recv, part_send, part_recv,
                    ring_send, ring_recv):
    chips = ep // 2
    tok, width = dyall.shape[1], dyall.shape[2]
    half = tok // 2
    n_exp, ff = wgt_v.shape[0], wgt_v.shape[1]
    top = topk_v.shape[0]
    pair = 2 * cap
    me = lax.axis_index('ep')
    chip, core = me // 2, me % 2
    right = (chip + 1) % chips
    left = (chip + chips - 1) % chips
    far = (chip + 2) % chips
    dev_r, dev_l, dev_p = right * 2 + core, left * 2 + core, chip * 2 + (1 - core)
    ahead = right * (1 - core) + left * core
    behind = left * (1 - core) + right * core
    dev_a = ahead * 2 + core
    home_of = (left * 2, right * 2, left * 2 + 1, right * 2 + 1, far * 2, far * 2 + 1, chip * 2, chip * 2 + 1)

    def remote(src, dst, send_sem, recv_sem, dev):
        return pltpu.make_async_remote_copy(src_ref=src, dst_ref=dst, send_sem=send_sem, recv_sem=recv_sem,
                                            device_id={'ep': dev}, device_id_type=MESH)

    def load(src, dst, i):
        return pltpu.make_async_copy(src, dst, load_sem.at[i])

    def by_rows(src, dst, i):
        return [pltpu.make_async_copy(src.at[:, pl.ds(pl.multiple_of(home_of[b] * cap, cap), cap), :],
                                      dst.at[:, pl.ds(b * cap, cap), :], row_sem.at[i, b]) for b in range(ep)]

    own_load = load(dy_hbm, dyall.at[me], 0)
    route_loads = [load(topk_hbm, topk_v, 1), load(slot_hbm, slot_v, 2),
                   load(gate_hbm, meta.at[me, pl.ds(top, top), :], 3)]
    h_loads = by_rows(h1_hbm, h1_v, 0) + by_rows(h3_hbm, h3_v, 1)
    wd_load, wg_load = load(wd_hbm, dyd_v, 4), load(wg_hbm, xt_v, 5)
    wu_loads = [load(wu_hbm.at[:, pl.ds(i * ff, ff), :], x_v.at[:, :, pl.ds(i * ff, ff)], 6 + i) for i in range(2)]
    yb_load = load(yb_hbm, yb_v, 8)
    x_loads = by_rows(x_hbm, x_v, 2)

    barrier = pltpu.get_barrier_semaphore()
    for d in range(1, ep):
        pl.semaphore_signal(barrier, inc=1, device_id={'ep': (me + d) % ep}, device_id_type=MESH)
    for copy in [own_load] + route_loads + [wd_load, wg_load]:
        copy.start()
    square[...] = jnp.zeros_like(square)
    for copy in route_loads:
        copy.wait()
    slot = slot_v[...]
    meta[me, 0:top, :] = jnp.where(slot >= 0, topk_v[...] * cap + slot, -1).astype(F32)
    own_load.wait()
    for copy in wu_loads:
        copy.start()
    pl.semaphore_wait(barrier, ep - 1)

    def rows(ref, home, h):
        return ref.at[home, pl.ds(pl.multiple_of(h * half, half), half), :]

    def dy_copy(home, h, send_sem, recv_sem, dev):
        return remote(rows(dyall, home, h), rows(dyall, home, h), send_sem, recv_sem, dev)

    own_a = dy_copy(me, 1 - core, d2d_send.at[0], d2d_recv.at[0], dev_p)
    own_b = dy_copy(me, core, d2d_send.at[1], d2d_recv.at[1], dev_p)
    to_r = [dy_copy(chip * 2 + q, core, dy_send.at[q], dy_recv.at[q], dev_r) for q in range(2)]
    to_l = [dy_copy(chip * 2 + q, core, dy_send.at[2 + q], dy_recv.at[2 + q], dev_l) for q in range(2)]
    hop = [dy_copy(behind * 2 + q, core, dy_send.at[4 + q], dy_recv.at[4 + q], dev_a) for q in range(2)]
    left_p = [dy_copy(left * 2 + q, core, d2d_send.at[2 + q], d2d_recv.at[2 + q], dev_p) for q in range(2)]
    right_p = [dy_copy(right * 2 + q, core, d2d_send.at[4 + q], d2d_recv.at[4 + q], dev_p) for q in range(2)]
    far_p = [dy_copy(far * 2 + q, core, d2d_send.at[6 + q], d2d_recv.at[6 + q], dev_p) for q in range(2)]
    m_r, m_l, m_p, m_f, m_lp, m_rp, m_fp = metas = [
        remote(meta.at[home], meta.at[home], meta_send.at[i], meta_recv.at[i], dev) for i, (home, dev) in enumerate((
            (me, dev_r), (me, dev_l), (me, dev_p), (dev_l, dev_r), (dev_l, dev_p), (dev_r, dev_p), (far * 2 + core, dev_p)))]

    def start_first():
        to_r[0].start()
        to_l[0].start()

    own_a.start()
    pl.when(core == 0)(start_first)
    for copy in (m_r, m_l, m_p, own_b):
        copy.start()
    for copy in h_loads:
        copy.start()

    def factors(k):
        span = slice(k * pair, (k + 1) * pair)

        def one_expert(e, carry):
            gate_f = h1_v[e, span, :].astype(F32)
            up_f = h3_v[e, span, :].astype(F32)
            sig = jax.nn.sigmoid(gate_f)
            silu_v[e, span, :] = gate_f * sig
            slope_v[e, span, :] = up_f * sig * (1.0 + gate_f * (1.0 - sig))
            return carry
        lax.fori_loop(0, n_exp, one_expert, 0)

    def activations(e, carry):
        for k in range(chips):
            span = slice(k * pair, (k + 1) * pair)
            actt_v[e, :, span] = (silu_v[e, span, :] * h3_v[e, span, :].astype(F32)).astype(BF16).T
        return carry

    def build(b):
        home = home_of[b]
        table = meta[home]
        row_id = lax.broadcasted_iota(jnp.int32, (n_exp * cap, tok), 0).astype(F32) + (me * (n_exp * cap)).astype(F32)
        hit = jnp.zeros((n_exp * cap, tok), F32)
        gate = jnp.zeros((n_exp * cap, tok), F32)
        for j in range(top):
            same = row_id == table[j:j + 1, :]
            hit = jnp.where(same, 1.0, hit)
            gate = jnp.where(same, table[top + j:top + j + 1, :], gate)
        gate_row = jnp.sum(gate, axis=1, keepdims=True)
        sel = hit.astype(BF16)
        onehot[b] = sel
        for n in range(width // 256):
            cols = slice(n * 256, (n + 1) * 256)
            block = (jnp.dot(sel, dyall[home, :, cols], preferred_element_type=F32) * gate_row).astype(BF16)
            for e in range(n_exp):
                dyd_v[e, b * cap:(b + 1) * cap, cols] = block[e * cap:(e + 1) * cap]

    def experts(k, between):
        span = slice(k * pair, (k + 1) * pair)
        for e in range(n_exp):
            d_act = jnp.dot(dyd_v[e, span, :], wdt_v[e], preferred_element_type=F32).astype(BF16).astype(F32)
            dh_v[e, span, 0:ff] = (d_act * slope_v[e, span, :]).astype(BF16)
            dh_v[e, span, ff:2 * ff] = (d_act * silu_v[e, span, :]).astype(BF16)
        between()
        for e in range(n_exp):
            out = (jnp.dot(dh_v[e, span, 0:ff], wgt_v[e], preferred_element_type=F32)
                   + jnp.dot(dh_v[e, span, ff:2 * ff], wut_v[e], preferred_element_type=F32)).astype(BF16)
            for j in range(2):
                dxd[k % 2, j, e * cap:(e + 1) * cap, :] = out[j * cap:(j + 1) * cap]

    def token_sum(k, j):
        return dot_tn(onehot[2 * k + j], dxd[k % 2, j])

    def piece(h):
        return pl.ds(pl.multiple_of(h * half, half), half)

    part_a = [remote(theirs.at[q, piece(core), :], got.at[q, piece(core), :], part_send.at[q], part_recv.at[q], dev_p)
              for q in range(2)]
    part_b = [remote(theirs.at[q, piece(1 - core), :], got.at[q, piece(1 - core), :], part_send.at[2 + q],
                     part_recv.at[2 + q], dev_p) for q in range(2)]
    part_f = [remote(fsum.at[q, piece(1 - core), :], fgot.at[q], part_send.at[4 + q], part_recv.at[4 + q], dev_p)
              for q in range(2)]
    part_o = remote(own.at[1], own.at[2], part_send.at[6], part_recv.at[6], dev_p)
    one = [remote(mine.at[q, piece(1 - core), :], final.at[core, piece(1 - core), :], ring_send.at[q], ring_recv.at[core],
                  ahead * 2 + q) for q in range(2)]
    two = [remote(fsum.at[q, piece(core), :], relay.at[q], ring_send.at[2 + q], ring_recv.at[2 + q], dev_a)
           for q in range(2)]
    three = [remote(mine.at[q, piece(core), :], final.at[core, piece(core), :], ring_send.at[4 + q],
                    ring_recv.at[4 + core], ahead * 2 + q) for q in range(2)]

    def landed(direction, h, sem):
        where = final.at[direction, pl.ds(h * half, half), :]
        remote(where, where, ring_send.at[0], ring_recv.at[sem], dev_p).wait_recv()

    def early_r():
        to_r[1].wait_recv()
        left_p[1].start()

    def early_l():
        to_l[1].wait_recv()
        right_p[1].start()

    def next_homes():
        pl.when(core == 0)(early_r)
        pl.when(core == 1)(early_l)
        hop[1].start()

    def late_homes():
        pl.when(core == 0)(early_l)
        pl.when(core == 1)(early_r)

    def send_one(q):
        part_a[q].wait_recv()
        at = piece(1 - core)
        mine[q, at, :] = mine[q, at, :] + got[q, at, :]
        one[q].start()

    def sums(q):
        theirs[q] = token_sum(q, core)
        mine[q] = token_sum(q, 1 - core)
        part_a[q].start()
        part_b[q].start()

    def turn_down(e, carry):
        wdt_v[e] = dyd_v[e].T
        return carry

    def turn_gate(e, carry):
        wgt_v[e] = xt_v[e].T
        return carry

    def turn_up(e, carry):
        for i in range(2):
            wut_v[e, :, i * ff:(i + 1) * ff] = x_v[e, :, i * ff:(i + 1) * ff].T
        return carry

    wd_load.wait()
    lax.fori_loop(0, n_exp // 2, turn_down, 0)
    own_a.wait_recv()
    pl.when(core == 1)(start_first)
    pl.when(core == 0)(to_r[1].start)
    pl.when(core == 1)(to_l[1].start)
    lax.fori_loop(n_exp // 2, n_exp, turn_down, 0)
    m_r.wait_recv()
    m_f.start()
    m_lp.start()
    m_l.wait_recv()
    m_rp.start()
    wg_load.wait()
    lax.fori_loop(0, n_exp, turn_gate, 0)
    to_r[0].wait_recv()
    left_p[0].start()
    to_l[0].wait_recv()
    right_p[0].start()
    hop[0].start()
    pl.when(core == 0)(to_l[1].start)
    pl.when(core == 1)(to_r[1].start)
    for copy in wu_loads:
        copy.wait()
    lax.fori_loop(0, n_exp, turn_up, 0)
    for copy in x_loads + [yb_load]:
        copy.start()
    for copy in h_loads:
        copy.wait()
    factors(0)

    m_lp.wait_recv()
    m_rp.wait_recv()
    left_p[0].wait_recv()
    right_p[0].wait_recv()
    build(0)
    build(1)
    next_homes()
    experts(0, lambda: None)
    sums(0)
    factors(1)
    late_homes()
    factors(2)
    factors(3)
    left_p[1].wait_recv()
    right_p[1].wait_recv()
    build(2)
    build(3)


    def far_homes():
        send_one(0)
        m_f.wait_recv()
        m_fp.start()
        for q in range(2):
            hop[q].wait_recv()
            far_p[q].start()

    experts(1, far_homes)
    sums(1)
    m_fp.wait_recv()
    for q in range(2):
        far_p[q].wait_recv()
    build(4)
    build(5)
    experts(2, lambda: send_one(1))
    for q in range(2):
        fsum[q] = token_sum(2, q)
    for q in range(2):
        part_f[q].start()

    def send_two():
        for q in range(2):
            part_f[q].wait_recv()
            at = piece(core)
            fsum[q, at, :] = fsum[q, at, :] + fgot[q]
            two[q].start()

    m_p.wait_recv()
    own_b.wait_recv()
    build(6)
    build(7)
    experts(3, send_two)
    own[1] = token_sum(3, 1 - core)
    own[0] = token_sum(3, core)
    part_o.start()
    for q in range(2):
        part_b[q].wait_recv()
        at = piece(core)
        mine[q, at, :] = mine[q, at, :] + got[q, at, :]

    lax.fori_loop(0, n_exp, activations, 0)
    yb_load.wait()

    def gate_grad(i, carry):
        at = pl.ds(pl.multiple_of(i * 16, 16), 16)
        prod = yb_v[at].astype(F32) * dyall[me, at, :].astype(F32)[:, None, :]
        square[at, 0:top] = jnp.sum(prod, axis=-1)
        return carry
    lax.fori_loop(0, tok // 16, gate_grad, 0)
    dg_ref[...] = square[...].T[0:top, :]
    part_o.wait_recv()
    own[0] = own[0] + own[2]

    for q in range(2):
        two[q].wait_recv()
        at = piece(core)
        mine[q, at, :] = mine[q, at, :] + relay[q]
        three[q].start()
    for copy in x_loads:
        copy.wait()

    def turn(e, carry):
        for p in range(chips):
            span = slice(p * pair, (p + 1) * pair)
            xt_v[e, :, span] = x_v[e, span, :].T
        return carry
    lax.fori_loop(0, n_exp, turn, 0)
    first_ref[...] = jnp.dot(actt_v[0], dyd_v[0], preferred_element_type=F32)
    landed(0, 1, 0)
    landed(1, 0, 1)
    landed(0, 0, 4)
    landed(1, 1, 5)
    dx_ref[...] = (own[0] + final[0] + final[1]).astype(BF16)

    for copy in metas + [own_a, own_b] + to_r + to_l + hop + left_p + right_p + far_p + part_a + part_b + part_f + [
            part_o] + one + two + three:
        copy.wait_send()


def exchange(ep, dy, topk, slot, gates, y_back, x, h1, h3, w_gate, w_up, w_down):
    tok, width = dy.shape
    n_exp, rows_e, ff = h1.shape
    cap = rows_e // ep
    top = topk.shape[0]
    any_spec = pl.BlockSpec(memory_space=pl.ANY)
    vmem_spec = pl.BlockSpec(memory_space=pltpu.VMEM)
    dma = pltpu.SemaphoreType.DMA
    return pl.pallas_call(
        functools.partial(exchange_kernel, ep, cap),
        out_shape=(
            pltpu.VMEM((tok, width), BF16),
            pltpu.VMEM((top, tok), F32),
            pltpu.VMEM((ff, width), F32),
            pltpu.VMEM((n_exp, width, rows_e), BF16),
            pltpu.VMEM((n_exp, rows_e, width), BF16),
            pltpu.VMEM((n_exp, ff, rows_e), BF16),
            pltpu.VMEM((n_exp, rows_e, 2 * ff), BF16),
        ),
        in_specs=[any_spec] * 11,
        out_specs=(vmem_spec,) * 7,
        scratch_shapes=[
            pltpu.VMEM((ep, tok, width), BF16),
            pltpu.VMEM((ep, 2 * top, tok), F32),
            pltpu.VMEM((top, tok), jnp.int32),
            pltpu.VMEM((top, tok), jnp.int32),
            pltpu.VMEM((tok, tok), F32),
            pltpu.VMEM((tok, top, width), BF16),
            pltpu.VMEM((n_exp, rows_e, width), BF16),
            pltpu.VMEM((n_exp, rows_e, ff), BF16),
            pltpu.VMEM((n_exp, rows_e, ff), BF16),
            pltpu.VMEM((n_exp, rows_e, ff), F32),
            pltpu.VMEM((n_exp, rows_e, ff), F32),
            pltpu.VMEM((n_exp, ff, width), BF16),
            pltpu.VMEM((n_exp, ff, width), BF16),
            pltpu.VMEM((n_exp, width, ff), BF16),
            pltpu.VMEM((ep, n_exp * cap, tok), BF16),
            pltpu.VMEM((2, 2, n_exp * cap, width), BF16),
            pltpu.VMEM((2, tok, width), F32),
            pltpu.VMEM((2, tok, width), F32),
            pltpu.VMEM((2, tok, width), F32),
            pltpu.VMEM((2, tok, width), F32),
            pltpu.VMEM((2, tok // 2, width), F32),
            pltpu.VMEM((3, tok, width), F32),
            pltpu.VMEM((2, tok // 2, width), F32),
            pltpu.VMEM((2, tok, width), F32),
            dma((9,)), dma((3, ep)), dma((7,)), dma((7,)), dma((6,)), dma((6,)), dma((8,)), dma((8,)),
            dma((7,)), dma((7,)), dma((6,)), dma((6,)),
        ],
        compiler_params=pltpu.CompilerParams(collective_id=0, has_side_effects=True, vmem_limit_bytes=44 * 2**20),
        name='exchange',
    )(dy, topk, slot, gates, y_back, x, h1, h3, w_gate, w_up, w_down)


def weight_grad_kernel(dx_v, dg_v, first_v, xt_v, dyd_v, actt_v, dh_v, dx_hbm, dg_hbm, dwg_hbm, dwu_hbm, dwd_hbm, stage, sem, small_sem):
    n_exp, width, _ = xt_v.shape
    ff = actt_v.shape[1]
    slots, block = stage.shape[0], stage.shape[1]
    down = ff // block
    units = [(u, e) for e in range(n_exp) for u in range((ff + width) // block)][ff // block:]
    small = [pltpu.make_async_copy(dx_v, dx_hbm, small_sem.at[0]), pltpu.make_async_copy(dg_v, dg_hbm, small_sem.at[1]),
             pltpu.make_async_copy(first_v, dwd_hbm.at[0], small_sem.at[2])]
    for copy in small[::-1]:
        copy.start()

    def copies(i):
        (u, e), s = units[i], i % slots
        if u < down:
            return [pltpu.make_async_copy(stage.at[s], dwd_hbm.at[e, pl.ds(u * block, block), :], sem.at[s, 0])]
        at = pl.ds((u - down) * block, block)
        return [pltpu.make_async_copy(stage.at[s, :, pl.ds(0, ff)], dwg_hbm.at[e, at, :], sem.at[s, 0]),
                pltpu.make_async_copy(stage.at[s, :, pl.ds(ff, ff)], dwu_hbm.at[e, at, :], sem.at[s, 1])]

    for i, (u, e) in enumerate(units):
        if i >= slots:
            for copy in copies(i - slots):
                copy.wait()
        if u < down:
            stage[i % slots] = jnp.dot(actt_v[e, u * block:(u + 1) * block, :], dyd_v[e], preferred_element_type=F32)
        else:
            at = slice((u - down) * block, (u - down + 1) * block)
            stage[i % slots] = jnp.dot(xt_v[e, at, :], dh_v[e], preferred_element_type=F32)
        for copy in copies(i):
            copy.start()
    for i in range(len(units) - slots, len(units)):
        for copy in copies(i):
            copy.wait()
    for copy in small:
        copy.wait()


def weight_grads(dx, d_gates, first, xt, dyd, actt, dh):
    n_exp, width, _ = xt.shape
    ff = actt.shape[1]
    block, slots = 512, 4
    any_spec = pl.BlockSpec(memory_space=pl.ANY)
    vmem_spec = pl.BlockSpec(memory_space=pltpu.VMEM)
    return pl.pallas_call(
        weight_grad_kernel,
        out_shape=(
            jax.ShapeDtypeStruct(dx.shape, dx.dtype),
            jax.ShapeDtypeStruct(d_gates.shape, d_gates.dtype),
            jax.ShapeDtypeStruct((n_exp, width, ff), F32),
            jax.ShapeDtypeStruct((n_exp, width, ff), F32),
            jax.ShapeDtypeStruct((n_exp, ff, width), F32),
        ),
        in_specs=[vmem_spec] * 7,
        out_specs=(any_spec,) * 5,
        scratch_shapes=[pltpu.VMEM((slots, block, width), F32), pltpu.SemaphoreType.DMA((slots, 2)),
                        pltpu.SemaphoreType.DMA((3,))],
        compiler_params=pltpu.CompilerParams(vmem_limit_bytes=20 * 2**20),
        cost_estimate=pl.CostEstimate(flops=6 * n_exp * xt.shape[2] * width * ff, transcendentals=0,
                                      bytes_accessed=12 * n_exp * width * ff),
        name='weight_grads',
    )(*[pltpu.with_memory_space_constraint(x, pltpu.VMEM) for x in (dx, d_gates, first, xt, dyd, actt, dh)])


def solution(mesh):
    ep = mesh.shape['ep']
    tok_spec = P(('dp', 'ep'), None)
    buf_spec = P(('dp', 'ep'), None, None)
    expert_spec = P('ep', None, None)

    def device_step(dy, topk_idx, slot_idx, gates, y_back, x_disp, h1_disp, h3_disp, w_gate, w_up, w_down):
        saved = exchange(
            ep, dy, topk_idx.T, slot_idx.T, gates.T, y_back, x_disp, h1_disp, h3_disp, w_gate, w_up, w_down)
        dx, d_gates, dw_gate, dw_up, dw_down = weight_grads(*saved)
        return dx, d_gates.T, dw_gate, dw_up, dw_down

    return jax.shard_map(
        device_step, mesh=mesh,
        in_specs=(tok_spec, tok_spec, tok_spec, tok_spec, buf_spec, buf_spec, buf_spec, buf_spec,
                  expert_spec, expert_spec, expert_spec),
        out_specs=(tok_spec, tok_spec, buf_spec, buf_spec, buf_spec),
        check_vma=False)
```

```python
import functools
import jax
import jax.numpy as jnp
from jax import lax
from jax.experimental import pallas as pl
from jax.experimental.pallas import tpu as pltpu
from jax.sharding import PartitionSpec as P

MESH = pl.DeviceIdType.MESH
F32 = jnp.float32
BF16 = jnp.bfloat16


def dot_tn(a, b):
    return lax.dot_general(a, b, (((0,), (0,)), ((), ())), preferred_element_type=F32)


def exchange_kernel(ep, cap, dy_hbm, topk_hbm, slot_hbm, gate_hbm, yb_hbm, x_hbm, h1_hbm, h3_hbm, wg_hbm, wu_hbm, wd_hbm,
                    acc_ref, same_ref, cross_ref, dg_ref, first_ref, xt_v, dyd_v, actt_v, dh_v,
                    dyall, meta, topk_v, slot_v, square, yb_v, x_v, h1_v, h3_v, silu_v, slope_v, wgt_v, wut_v, wdt_v,
                    onehot, dxd, mine, theirs, got, fsum, fgot, own, relay, final,
                    load_sem, row_sem, meta_send, meta_recv, dy_send, dy_recv, d2d_send, d2d_recv, part_send, part_recv,
                    ring_send, ring_recv):
    chips = ep // 2
    tok, width = dyall.shape[1], dyall.shape[2]
    half = tok // 2
    n_exp, ff = wgt_v.shape[0], wgt_v.shape[1]
    top = topk_v.shape[0]
    pair = 2 * cap
    me = lax.axis_index('ep')
    chip, core = me // 2, me % 2
    right = (chip + 1) % chips
    left = (chip + chips - 1) % chips
    far = (chip + 2) % chips
    dev_r, dev_l, dev_p = right * 2 + core, left * 2 + core, chip * 2 + (1 - core)
    ahead = right * (1 - core) + left * core
    behind = left * (1 - core) + right * core
    dev_a = ahead * 2 + core
    home_of = (left * 2, right * 2, left * 2 + 1, right * 2 + 1, far * 2, far * 2 + 1, chip * 2, chip * 2 + 1)

    def remote(src, dst, send_sem, recv_sem, dev):
        return pltpu.make_async_remote_copy(src_ref=src, dst_ref=dst, send_sem=send_sem, recv_sem=recv_sem,
                                            device_id={'ep': dev}, device_id_type=MESH)

    def load(src, dst, i):
        return pltpu.make_async_copy(src, dst, load_sem.at[i])

    def by_rows(src, dst, i):
        return [pltpu.make_async_copy(src.at[:, pl.ds(pl.multiple_of(home_of[b] * cap, cap), cap), :],
                                      dst.at[:, pl.ds(b * cap, cap), :], row_sem.at[i, b]) for b in range(ep)]

    own_load = load(dy_hbm, dyall.at[me], 0)
    route_loads = [load(topk_hbm, topk_v, 1), load(slot_hbm, slot_v, 2),
                   load(gate_hbm, meta.at[me, pl.ds(top, top), :], 3)]
    h_loads = by_rows(h1_hbm, h1_v, 0) + by_rows(h3_hbm, h3_v, 1)
    wd_load, wg_load = load(wd_hbm, dyd_v, 4), load(wg_hbm, xt_v, 5)
    wu_loads = [load(wu_hbm.at[:, pl.ds(i * ff, ff), :], x_v.at[:, :, pl.ds(i * ff, ff)], 6 + i) for i in range(2)]
    yb_load = load(yb_hbm, yb_v, 8)
    x_loads = by_rows(x_hbm, x_v, 2)

    barrier = pltpu.get_barrier_semaphore()
    for d in range(1, ep):
        pl.semaphore_signal(barrier, inc=1, device_id={'ep': (me + d) % ep}, device_id_type=MESH)
    for copy in [own_load] + route_loads + [wd_load, wg_load]:
        copy.start()
    square[...] = jnp.zeros_like(square)
    for copy in route_loads:
        copy.wait()
    slot = slot_v[...]
    meta[me, 0:top, :] = jnp.where(slot >= 0, topk_v[...] * cap + slot, -1).astype(F32)
    own_load.wait()
    for copy in wu_loads:
        copy.start()
    pl.semaphore_wait(barrier, ep - 1)

    def rows(ref, home, h):
        return ref.at[home, pl.ds(pl.multiple_of(h * half, half), half), :]

    def dy_copy(home, h, send_sem, recv_sem, dev):
        return remote(rows(dyall, home, h), rows(dyall, home, h), send_sem, recv_sem, dev)

    own_a = dy_copy(me, 1 - core, d2d_send.at[0], d2d_recv.at[0], dev_p)
    own_b = dy_copy(me, core, d2d_send.at[1], d2d_recv.at[1], dev_p)
    to_r = [dy_copy(chip * 2 + q, core, dy_send.at[q], dy_recv.at[q], dev_r) for q in range(2)]
    to_l = [dy_copy(chip * 2 + q, core, dy_send.at[2 + q], dy_recv.at[2 + q], dev_l) for q in range(2)]
    hop = [dy_copy(behind * 2 + q, core, dy_send.at[4 + q], dy_recv.at[4 + q], dev_a) for q in range(2)]
    left_p = [dy_copy(left * 2 + q, core, d2d_send.at[2 + q], d2d_recv.at[2 + q], dev_p) for q in range(2)]
    right_p = [dy_copy(right * 2 + q, core, d2d_send.at[4 + q], d2d_recv.at[4 + q], dev_p) for q in range(2)]
    far_p = [dy_copy(far * 2 + q, core, d2d_send.at[6 + q], d2d_recv.at[6 + q], dev_p) for q in range(2)]
    m_r, m_l, m_p, m_f, m_lp, m_rp, m_fp = metas = [
        remote(meta.at[home], meta.at[home], meta_send.at[i], meta_recv.at[i], dev) for i, (home, dev) in enumerate((
            (me, dev_r), (me, dev_l), (me, dev_p), (dev_l, dev_r), (dev_l, dev_p), (dev_r, dev_p), (far * 2 + core, dev_p)))]

    def start_first():
        to_r[0].start()
        to_l[0].start()

    own_a.start()
    pl.when(core == 0)(start_first)
    for copy in (m_r, m_l, m_p, own_b):
        copy.start()
    for copy in h_loads:
        copy.start()

    def factors(k):
        span = slice(k * pair, (k + 1) * pair)

        def one_expert(e, carry):
            gate_f = h1_v[e, span, :].astype(F32)
            up_f = h3_v[e, span, :].astype(F32)
            sig = jax.nn.sigmoid(gate_f)
            silu_v[e, span, :] = gate_f * sig
            slope_v[e, span, :] = up_f * sig * (1.0 + gate_f * (1.0 - sig))
            return carry
        lax.fori_loop(0, n_exp, one_expert, 0)

    def activations(e, carry):
        for k in range(chips):
            span = slice(k * pair, (k + 1) * pair)
            actt_v[e, :, span] = (silu_v[e, span, :] * h3_v[e, span, :].astype(F32)).astype(BF16).T
        return carry

    def build(b):
        home = home_of[b]
        table = meta[home]
        row_id = lax.broadcasted_iota(jnp.int32, (n_exp * cap, tok), 0).astype(F32) + (me * (n_exp * cap)).astype(F32)
        hit = jnp.zeros((n_exp * cap, tok), F32)
        gate = jnp.zeros((n_exp * cap, tok), F32)
        for j in range(top):
            same = row_id == table[j:j + 1, :]
            hit = jnp.where(same, 1.0, hit)
            gate = jnp.where(same, table[top + j:top + j + 1, :], gate)
        gate_row = jnp.sum(gate, axis=1, keepdims=True)
        sel = hit.astype(BF16)
        onehot[b] = sel
        for n in range(width // 256):
            cols = slice(n * 256, (n + 1) * 256)
            block = (jnp.dot(sel, dyall[home, :, cols], preferred_element_type=F32) * gate_row).astype(BF16)
            for e in range(n_exp):
                dyd_v[e, b * cap:(b + 1) * cap, cols] = block[e * cap:(e + 1) * cap]

    def experts(k, between):
        span = slice(k * pair, (k + 1) * pair)
        for e in range(n_exp):
            d_act = jnp.dot(dyd_v[e, span, :], wdt_v[e], preferred_element_type=F32).astype(BF16).astype(F32)
            dh_v[e, span, 0:ff] = (d_act * slope_v[e, span, :]).astype(BF16)
            dh_v[e, span, ff:2 * ff] = (d_act * silu_v[e, span, :]).astype(BF16)
        between()
        for e in range(n_exp):
            out = (jnp.dot(dh_v[e, span, 0:ff], wgt_v[e], preferred_element_type=F32)
                   + jnp.dot(dh_v[e, span, ff:2 * ff], wut_v[e], preferred_element_type=F32)).astype(BF16)
            for j in range(2):
                dxd[k % 2, j, e * cap:(e + 1) * cap, :] = out[j * cap:(j + 1) * cap]

    def token_sum(k, j):
        return dot_tn(onehot[2 * k + j], dxd[k % 2, j])

    def piece(h):
        return pl.ds(pl.multiple_of(h * half, half), half)

    part_a = [remote(theirs.at[q, piece(core), :], got.at[q, piece(core), :], part_send.at[q], part_recv.at[q], dev_p)
              for q in range(2)]
    part_b = [remote(theirs.at[q, piece(1 - core), :], got.at[q, piece(1 - core), :], part_send.at[2 + q],
                     part_recv.at[2 + q], dev_p) for q in range(2)]
    part_f = [remote(fsum.at[q, piece(1 - core), :], fgot.at[q], part_send.at[4 + q], part_recv.at[4 + q], dev_p)
              for q in range(2)]
    part_o = remote(own.at[1], own.at[2], part_send.at[6], part_recv.at[6], dev_p)
    one = [remote(mine.at[q, piece(1 - core), :], final.at[core, piece(1 - core), :], ring_send.at[q], ring_recv.at[core],
                  ahead * 2 + q) for q in range(2)]
    two = [remote(fsum.at[q, piece(core), :], relay.at[q], ring_send.at[2 + q], ring_recv.at[2 + q], dev_a)
           for q in range(2)]

    first, last = slice(0, half), slice(half, tok)

    def landed(direction, h, sem):
        where = final.at[direction, pl.ds(h * half, half), :]
        remote(where, where, ring_send.at[0], ring_recv.at[sem], dev_p).wait_recv()

    def early_r():
        to_r[1].wait_recv()
        left_p[1].start()

    def early_l():
        to_l[1].wait_recv()
        right_p[1].start()

    def next_homes():
        pl.when(core == 0)(early_r)
        pl.when(core == 1)(early_l)
        hop[1].start()

    def late_homes():
        pl.when(core == 0)(early_l)
        pl.when(core == 1)(early_r)

    def send_one(q):
        part_a[q].wait_recv()
        at = piece(1 - core)
        mine[q, at, :] = mine[q, at, :] + got[q, at, :]
        one[q].start()

    def sums(q):
        theirs[q] = token_sum(q, core)
        mine[q] = token_sum(q, 1 - core)
        part_a[q].start()
        part_b[q].start()

    def turn_down(e, carry):
        wdt_v[e] = dyd_v[e].T
        return carry

    def turn_gate(e, carry):
        wgt_v[e] = xt_v[e].T
        return carry

    def turn_up(e, carry):
        for i in range(2):
            wut_v[e, :, i * ff:(i + 1) * ff] = x_v[e, :, i * ff:(i + 1) * ff].T
        return carry

    wd_load.wait()
    lax.fori_loop(0, n_exp // 2, turn_down, 0)
    own_a.wait_recv()
    pl.when(core == 1)(start_first)
    pl.when(core == 0)(to_r[1].start)
    pl.when(core == 1)(to_l[1].start)
    lax.fori_loop(n_exp // 2, n_exp, turn_down, 0)
    m_r.wait_recv()
    m_f.start()
    m_lp.start()
    m_l.wait_recv()
    m_rp.start()
    wg_load.wait()
    lax.fori_loop(0, n_exp, turn_gate, 0)
    to_r[0].wait_recv()
    left_p[0].start()
    to_l[0].wait_recv()
    right_p[0].start()
    hop[0].start()
    pl.when(core == 0)(to_l[1].start)
    pl.when(core == 1)(to_r[1].start)
    for copy in wu_loads:
        copy.wait()
    lax.fori_loop(0, n_exp, turn_up, 0)
    for copy in x_loads + [yb_load]:
        copy.start()
    for copy in h_loads:
        copy.wait()
    factors(0)

    m_lp.wait_recv()
    m_rp.wait_recv()
    left_p[0].wait_recv()
    right_p[0].wait_recv()
    build(0)
    build(1)
    next_homes()
    experts(0, lambda: None)
    sums(0)
    factors(1)
    late_homes()
    factors(2)
    factors(3)
    left_p[1].wait_recv()
    right_p[1].wait_recv()
    build(2)
    build(3)


    def far_homes():
        send_one(0)
        m_f.wait_recv()
        m_fp.start()
        for q in range(2):
            hop[q].wait_recv()
            far_p[q].start()

    experts(1, far_homes)
    sums(1)
    m_fp.wait_recv()
    for q in range(2):
        far_p[q].wait_recv()
    build(4)
    build(5)
    experts(2, lambda: send_one(1))
    for q in range(2):
        fsum[q] = token_sum(2, q)
    for q in range(2):
        part_f[q].start()

    def send_two():
        for q in range(2):
            part_f[q].wait_recv()
            at = piece(core)
            fsum[q, at, :] = fsum[q, at, :] + fgot[q]
            two[q].start()

    m_p.wait_recv()
    own_b.wait_recv()
    build(6)
    build(7)
    experts(3, send_two)
    own[1] = token_sum(3, 1 - core)
    own[0] = token_sum(3, core)
    part_o.start()
    for q in range(2):
        part_b[q].wait_recv()
        at = piece(core)
        mine[q, at, :] = mine[q, at, :] + got[q, at, :]

    lax.fori_loop(0, n_exp, activations, 0)
    yb_load.wait()

    def gate_grad(i, carry):
        at = pl.ds(pl.multiple_of(i * 16, 16), 16)
        prod = yb_v[at].astype(F32) * dyall[me, at, :].astype(F32)[:, None, :]
        square[at, 0:top] = jnp.sum(prod, axis=-1)
        return carry
    lax.fori_loop(0, tok // 16, gate_grad, 0)
    dg_ref[...] = square[...].T[0:top, :]
    part_o.wait_recv()
    own[0] = own[0] + own[2]

    for copy in x_loads:
        copy.wait()

    def turn(e, carry):
        for p in range(chips):
            span = slice(p * pair, (p + 1) * pair)
            xt_v[e, :, span] = x_v[e, span, :].T
        return carry
    lax.fori_loop(0, n_exp, turn, 0)
    first_ref[...] = jnp.dot(actt_v[0], dyd_v[0], preferred_element_type=F32)
    landed(0, 1, 0)
    landed(1, 0, 1)
    acc_ref[first, :] = own[0, first, :] + final[1, first, :]
    acc_ref[last, :] = own[0, last, :] + final[0, last, :]
    for q in range(2):
        two[q].wait_recv()
        got[q, first, :] = mine[q, piece(core), :] + relay[q]
    same_ref[...] = got[core, first, :]
    cross_ref[...] = got[1 - core, first, :]

    for copy in metas + [own_a, own_b] + to_r + to_l + hop + left_p + right_p + far_p + part_a + part_b + part_f + [
            part_o] + one + two:
        copy.wait_send()


def exchange(ep, dy, topk, slot, gates, y_back, x, h1, h3, w_gate, w_up, w_down):
    tok, width = dy.shape
    n_exp, rows_e, ff = h1.shape
    cap = rows_e // ep
    top = topk.shape[0]
    any_spec = pl.BlockSpec(memory_space=pl.ANY)
    vmem_spec = pl.BlockSpec(memory_space=pltpu.VMEM)
    dma = pltpu.SemaphoreType.DMA
    return pl.pallas_call(
        functools.partial(exchange_kernel, ep, cap),
        out_shape=(
            pltpu.VMEM((tok, width), F32),
            pltpu.VMEM((tok // 2, width), F32),
            pltpu.VMEM((tok // 2, width), F32),
            pltpu.VMEM((top, tok), F32),
            pltpu.VMEM((ff, width), F32),
            pltpu.VMEM((n_exp, width, rows_e), BF16),
            pltpu.VMEM((n_exp, rows_e, width), BF16),
            pltpu.VMEM((n_exp, ff, rows_e), BF16),
            pltpu.VMEM((n_exp, rows_e, 2 * ff), BF16),
        ),
        in_specs=[any_spec] * 11,
        out_specs=(vmem_spec,) * 9,
        scratch_shapes=[
            pltpu.VMEM((ep, tok, width), BF16),
            pltpu.VMEM((ep, 2 * top, tok), F32),
            pltpu.VMEM((top, tok), jnp.int32),
            pltpu.VMEM((top, tok), jnp.int32),
            pltpu.VMEM((tok, tok), F32),
            pltpu.VMEM((tok, top, width), BF16),
            pltpu.VMEM((n_exp, rows_e, width), BF16),
            pltpu.VMEM((n_exp, rows_e, ff), BF16),
            pltpu.VMEM((n_exp, rows_e, ff), BF16),
            pltpu.VMEM((n_exp, rows_e, ff), F32),
            pltpu.VMEM((n_exp, rows_e, ff), F32),
            pltpu.VMEM((n_exp, ff, width), BF16),
            pltpu.VMEM((n_exp, ff, width), BF16),
            pltpu.VMEM((n_exp, width, ff), BF16),
            pltpu.VMEM((ep, n_exp * cap, tok), BF16),
            pltpu.VMEM((2, 2, n_exp * cap, width), BF16),
            pltpu.VMEM((2, tok, width), F32),
            pltpu.VMEM((2, tok, width), F32),
            pltpu.VMEM((2, tok, width), F32),
            pltpu.VMEM((2, tok, width), F32),
            pltpu.VMEM((2, tok // 2, width), F32),
            pltpu.VMEM((3, tok, width), F32),
            pltpu.VMEM((2, tok // 2, width), F32),
            pltpu.VMEM((2, tok, width), F32),
            dma((9,)), dma((3, ep)), dma((7,)), dma((7,)), dma((6,)), dma((6,)), dma((8,)), dma((8,)),
            dma((7,)), dma((7,)), dma((6,)), dma((6,)),
        ],
        compiler_params=pltpu.CompilerParams(collective_id=0, has_side_effects=True, vmem_limit_bytes=44 * 2**20),
        name='exchange',
    )(dy, topk, slot, gates, y_back, x, h1, h3, w_gate, w_up, w_down)


def weight_grad_kernel(dg_v, first_v, xt_v, dyd_v, actt_v, dh_v, dg_hbm, dwg_hbm, dwu_hbm, dwd_hbm, stage, sem, small_sem):
    n_exp, width, _ = xt_v.shape
    ff = actt_v.shape[1]
    slots, block = stage.shape[0], stage.shape[1]
    down = ff // block
    units = [(u, e) for e in range(n_exp) for u in range((ff + width) // block)][ff // block:]
    small = [pltpu.make_async_copy(dg_v, dg_hbm, small_sem.at[1]),
             pltpu.make_async_copy(first_v, dwd_hbm.at[0], small_sem.at[2])]
    for copy in small[::-1]:
        copy.start()

    def copies(i):
        (u, e), s = units[i], i % slots
        if u < down:
            return [pltpu.make_async_copy(stage.at[s], dwd_hbm.at[e, pl.ds(u * block, block), :], sem.at[s, 0])]
        at = pl.ds((u - down) * block, block)
        return [pltpu.make_async_copy(stage.at[s, :, pl.ds(0, ff)], dwg_hbm.at[e, at, :], sem.at[s, 0]),
                pltpu.make_async_copy(stage.at[s, :, pl.ds(ff, ff)], dwu_hbm.at[e, at, :], sem.at[s, 1])]

    for i, (u, e) in enumerate(units):
        if i >= slots:
            for copy in copies(i - slots):
                copy.wait()
        if u < down:
            stage[i % slots] = jnp.dot(actt_v[e, u * block:(u + 1) * block, :], dyd_v[e], preferred_element_type=F32)
        else:
            at = slice((u - down) * block, (u - down + 1) * block)
            stage[i % slots] = jnp.dot(xt_v[e, at, :], dh_v[e], preferred_element_type=F32)
        for copy in copies(i):
            copy.start()
    for i in range(len(units) - slots, len(units)):
        for copy in copies(i):
            copy.wait()
    for copy in small:
        copy.wait()


def weight_grads(d_gates, first, xt, dyd, actt, dh):
    n_exp, width, _ = xt.shape
    ff = actt.shape[1]
    block, slots = 512, 4
    any_spec = pl.BlockSpec(memory_space=pl.ANY)
    vmem_spec = pl.BlockSpec(memory_space=pltpu.VMEM)
    return pl.pallas_call(
        weight_grad_kernel,
        out_shape=(
            jax.ShapeDtypeStruct(d_gates.shape, d_gates.dtype),
            jax.ShapeDtypeStruct((n_exp, width, ff), F32),
            jax.ShapeDtypeStruct((n_exp, width, ff), F32),
            jax.ShapeDtypeStruct((n_exp, ff, width), F32),
        ),
        in_specs=[vmem_spec] * 6,
        out_specs=(any_spec,) * 4,
        scratch_shapes=[pltpu.VMEM((slots, block, width), F32), pltpu.SemaphoreType.DMA((slots, 2)),
                        pltpu.SemaphoreType.DMA((3,))],
        compiler_params=pltpu.CompilerParams(vmem_limit_bytes=20 * 2**20),
        cost_estimate=pl.CostEstimate(flops=6 * n_exp * xt.shape[2] * width * ff, transcendentals=0,
                                      bytes_accessed=12 * n_exp * width * ff),
        name='weight_grads',
    )(*[pltpu.with_memory_space_constraint(x, pltpu.VMEM) for x in (d_gates, first, xt, dyd, actt, dh)])


def solution(mesh):
    ep = mesh.shape['ep']
    tok_spec = P(('dp', 'ep'), None)
    buf_spec = P(('dp', 'ep'), None, None)
    expert_spec = P('ep', None, None)

    def device_step(dy, topk_idx, slot_idx, gates, y_back, x_disp, h1_disp, h3_disp, w_gate, w_up, w_down):
        acc, same, cross, *saved = exchange(
            ep, dy, topk_idx.T, slot_idx.T, gates.T, y_back, x_disp, h1_disp, h3_disp, w_gate, w_up, w_down)
        ring = range(0, ep, 2)
        same = lax.ppermute(same, 'ep', [(i, (i + 2) % ep) for i in ring] + [(i + 1, (i + 1 - 2) % ep) for i in ring])
        cross = lax.ppermute(cross, 'ep', [(i, (i + 3) % ep) for i in ring] + [(i + 1, (i + ep - 2) % ep) for i in ring])
        d_gates, dw_gate, dw_up, dw_down = weight_grads(*saved)
        swap = lax.axis_index('ep') % 2 == 1
        halves = jnp.stack([jnp.where(swap, cross, same), jnp.where(swap, same, cross)])
        dx = (acc + halves.reshape(acc.shape)).astype(BF16)
        return dx, d_gates.T, dw_gate, dw_up, dw_down

    return jax.shard_map(
        device_step, mesh=mesh,
        in_specs=(tok_spec, tok_spec, tok_spec, tok_spec, buf_spec, buf_spec, buf_spec, buf_spec,
                  expert_spec, expert_spec, expert_spec),
        out_specs=(tok_spec, tok_spec, buf_spec, buf_spec, buf_spec),
        check_vma=False)
```
